256 devices in a mesh: interval: 4 (over z_lo, core), rows: 64 (over z_hi, x, y).
Axes of the slice: x: 4, y: 4, z: 8 (z_hi: 4, z_lo: 2; z = z_hi * 2 + z_lo), core: 2. Of those that a mesh axis runs over, the one named last changes fastest.
Arguments:
- filtered: float32 [4, 64, 1048576], P('interval', None, 'rows'), may hold values from -60 to 60, as said below
- potential: float32 [128, 64, 128], P('rows'), may hold values from 0.5 to 4
Outputs:
- basis: float32 [4, 64, 1048576], P('interval', None, 'rows')
- ritz_matrix: float32 [4, 64, 64], P('interval')
- ritz_residual: float32 [4, 64, 1048576], P('interval', None, 'rows')
The draws below stay inside these ranges and needn't reach their ends.
Inputs may be any that keep to these rules, and one draw needn't show every extreme that they name: `filtered`: the rows of each interval's block are linearly independent, and each interval's block shares a part with the block of the interval before it.
All inputs are finite; a program needn't handle non-finite values.
Results may differ from the reference program's by a relative error of at most 0.0003.
Values sent between devices are 32-bit elements; how exact they have to be, the bound alone decides.
A program may use at most 64 MiB of HBM per device.

```python
import math
import jax
import jax.numpy as jnp
from jax import lax

M = 64
GY = 64
GZ = 128
INTERVALS = 4
NX = 128
N = 1048576


def draw_filtered(key, part):
    keys = jax.random.split(jax.random.fold_in(key, 11), 3)
    base = jax.random.normal(keys[0], (INTERVALS, M, N), jnp.float32)
    mixing = jax.random.normal(keys[1], (INTERVALS, M, M), jnp.float32) / math.sqrt(M)
    earlier = jnp.roll(base, 1, axis=0)
    mixed = base + 0.6 * jnp.einsum('imk,ikn->imn', mixing, earlier)
    scales = jnp.exp(jax.random.uniform(keys[2], (INTERVALS, M, 1), jnp.float32, 0.0, math.log(10.0)))
    plane = jnp.arange(N) // (GY * GZ)
    ramp = jnp.exp(math.log(3.0) * plane.astype(jnp.float32) / max(NX - 1, 1))
    return jnp.clip(mixed * scales * ramp[None, None, :], -60.0, 60.0).astype(jnp.float32)


def steps_of(own_key, shape, pieces, low, high):
    gain = 1.0
    for dim, blocks in pieces:
        draws = jax.random.uniform(jax.random.fold_in(jax.random.fold_in(own_key, 6), dim), (blocks,), jnp.float32, low / len(pieces), high / len(pieces))
        gain = gain * jnp.repeat(jnp.exp(draws), shape[dim] // blocks).reshape((-1,) + (1,) * (len(shape) - 1 - dim))
    return gain


def setup_inputs(seed: int = 0) -> dict:
    seeds = jax.random.split(jax.random.key(seed), 3)
    filtered = draw_filtered(jax.random.fold_in(seeds[2], 71), 0)
    potential = jnp.clip(jnp.exp(math.log(4.0) - 2.0794415 * jax.random.uniform(seeds[1], (NX, GY, GZ), jnp.float32) ** steps_of(seeds[1], (NX, GY, GZ), ((0, 64),), -0.2, 0.2)), 0.5, 4.0)
    return {"filtered": filtered, "potential": potential}


def inner(left, right):
    return lax.dot_general(left.astype(jnp.float32), right.astype(jnp.float32), (((1,), (1,)), ((), ())), precision=lax.Precision.HIGHEST, preferred_element_type=jnp.float32)

def apply_left(matrix, vectors):
    return jnp.dot(matrix.astype(jnp.float32), vectors.astype(jnp.float32), precision=lax.Precision.HIGHEST, preferred_element_type=jnp.float32)

def orthonormal(vectors):
    lower = jnp.linalg.cholesky(inner(vectors, vectors))
    return lax.linalg.triangular_solve(lower, vectors, left_side=True, lower=True)

def operate(field, potential):
    padded = jnp.pad(field, ((0, 0), (1, 1), (1, 1), (1, 1)))
    beside = padded[:, 2:, 1:-1, 1:-1] + padded[:, :-2, 1:-1, 1:-1]
    beside = beside + padded[:, 1:-1, 2:, 1:-1] + padded[:, 1:-1, :-2, 1:-1]
    beside = beside + padded[:, 1:-1, 1:-1, 2:] + padded[:, 1:-1, 1:-1, :-2]
    return (6.0 + potential) * field - beside

def reference(filtered, potential):
    count = filtered.shape[0]
    width = filtered.shape[1]
    owns = [orthonormal(filtered[index]) for index in range(count)]
    bases = []
    matrices = []
    residuals = []
    for index in range(count):
        own = owns[index]
        if index == 0:
            prior = jnp.zeros_like(own)
        else:
            prior = owns[index - 1]
        cross = inner(own, prior)
        reduced = own - apply_left(cross, prior)
        basis = orthonormal(reduced)
        image = operate(basis.reshape(width, NX, GY, GZ), potential).reshape(width, -1)
        ritz_matrix = inner(basis, image)
        residual = image - apply_left(ritz_matrix.T, basis)
        bases.append(basis)
        matrices.append(ritz_matrix)
        residuals.append(residual)
    return (jnp.stack(bases), jnp.stack(matrices), jnp.stack(residuals))
```

```python
import jax
import jax.numpy as jnp
from jax import lax
from jax.experimental import pallas as pl
from jax.experimental.pallas import tpu as pltpu
from jax.sharding import PartitionSpec as P

MESH = pl.DeviceIdType.MESH
F32 = jnp.float32
BF16 = jnp.bfloat16

LANES = 128
LAYER = 16
CHUNKS = 8
RELAYS = (3, 7, 11, 4, 8, 12, 6, 9)


def split(v):
    hi = v.astype(BF16)
    return hi, (v - hi.astype(F32)).astype(BF16)


def exact_dot(a, b, dims):
    return lax.dot_general(
        a, b, (dims, ((), ())), precision=lax.Precision.HIGHEST, preferred_element_type=F32
    )


def stencil(u, low, high, pot, plane, j, size, width):
    base = plane * size
    start = pl.multiple_of(base + j * width, LANES)
    c = u[:, pl.ds(start, width)]
    first = pl.multiple_of(jnp.maximum(start - LANES, base), LANES)
    last = pl.multiple_of(jnp.minimum(start + width, base + size - LANES), LANES)
    before = jnp.where(j > 0, u[:, pl.ds(first, LANES)], 0.0)
    after = jnp.where(j < size // width - 1, u[:, pl.ds(last, LANES)], 0.0)
    tiles = width // LANES
    part = [c[:, t * LANES : (t + 1) * LANES] for t in range(tiles)]
    around = [before, *part, after]
    lane = lax.broadcasted_iota(jnp.int32, part[0].shape, 1)
    other = u[:, pl.ds(pl.multiple_of((1 - plane) * size + j * width, LANES), width)]
    halo = (high if plane else low)[:, pl.ds(pl.multiple_of(j * width, LANES), width)]
    weight = 6.0 + pot[:, pl.ds(start, width)]
    out = []
    for t in range(tiles):
        cut = slice(t * LANES, (t + 1) * LANES)
        left = jnp.where(lane == 0, 0.0, pltpu.roll(part[t], 1, 1))
        right = jnp.where(lane == LANES - 1, 0.0, pltpu.roll(part[t], LANES - 1, 1))
        beside = (other[:, cut] + halo[:, cut]) + (around[t] + around[t + 2]) + (left + right)
        out.append(weight[:, cut] * part[t] - beside)
    return jnp.concatenate(out, axis=1)


def inverse_factor(square):
    n = square.shape[0]
    row = lax.broadcasted_iota(jnp.int32, (n, LANES), 0)
    lane = lax.broadcasted_iota(jnp.int32, (n, LANES), 1)
    t = jnp.where(lane < n, square, jnp.where(lane == row + n, 1.0, 0.0))
    for k in range(n):
        pivot = t[k : k + 1, :]
        scaled = pivot * (1.0 / t[k : k + 1, k : k + 1])
        column = jnp.where(row > k, jnp.broadcast_to(t[:, k : k + 1], (n, LANES)), 0.0)
        t = t - column * scaled
    diagonal = jnp.sum(jnp.where(lane == row, t, 0.0), axis=1, keepdims=True)
    t = t * (1.0 / jnp.sqrt(diagonal))
    return pltpu.roll(t, LANES - n, 1)[:, :n]


def coefficients(total, prior, w_out, r_out):
    n = total.shape[0] // 2
    swapped = pltpu.roll(total, n, 1)
    gram, k_own = total[:n, :n], swapped[:n, :n]
    g_pi, k_pi = total[n:, :n], swapped[n:, :n]
    k_prior = pltpu.roll(prior, n, 1)[:, :n]
    inv_p = inverse_factor(prior)
    et = exact_dot(inv_p, g_pi, ((1,), (0,)))
    schur = gram - exact_dot(et, et, ((0,), (0,)))
    wide = jnp.concatenate([schur, jnp.zeros_like(schur)], axis=1)
    a = inverse_factor(wide)
    b = -exact_dot(a, exact_dot(et, inv_p, ((0,), (0,))), ((1,), (0,)))
    mixed = exact_dot(exact_dot(b, k_pi, ((1,), (0,))), a, ((1,), (1,)))
    mixed_t = exact_dot(a, exact_dot(b, k_pi, ((1,), (0,))), ((1,), (1,)))
    ritz = exact_dot(exact_dot(a, k_own, ((1,), (0,))), a, ((1,), (1,)))
    ritz = ritz + mixed + mixed_t
    ritz = ritz + exact_dot(exact_dot(b, k_prior, ((1,), (0,))), b, ((1,), (1,)))
    r_out[...] = ritz
    ra = exact_dot(ritz, a, ((0,), (0,)))
    rb = exact_dot(ritz, b, ((0,), (0,)))
    zero = jnp.zeros_like(a)
    w_out[:n, :] = jnp.concatenate([a, b, zero, zero], axis=1)
    w_out[n:, :] = jnp.concatenate([-ra, -rb, a, b], axis=1)


def exchange_kernel(
    intervals, rows,
    x, pot,
    prev_o, low_o, high_o, plow_o, phigh_o, w_o, r_o,
    prev, low, high, up_a, up_b, down_a, down_b, acc, sums, total, prior,
    x_send, x_recv, up_send, down_send, low_recv, high_recv,
    relay_send, relay_recv, plow_send, phigh_send, plow_recv, phigh_recv,
    out_sem, sum_send, sum_recv, prior_send, prior_recv,
):
    i, r = lax.axis_index("interval"), lax.axis_index("rows")
    layers = rows // LAYER
    layer, q = r // LAYER, r % LAYER
    qx, qy = q // 4, q % 4
    size = low.shape[1]
    width = size // CHUNKS

    def at(c):
        return pl.ds(pl.multiple_of(c * width, LANES), width)

    def remote(src, dst, send, recv, to_i, to_r):
        return pltpu.make_async_remote_copy(
            src_ref=src, dst_ref=dst, send_sem=send, recv_sem=recv,
            device_id=(to_i, to_r), device_id_type=MESH,
        )

    barrier = pltpu.get_barrier_semaphore()

    def greet(to_i, to_r):
        pl.semaphore_signal(barrier, inc=1, device_id=(to_i, to_r), device_id_type=MESH)

    for d in range(1, layers):
        greet(i, lax.rem(layer + d, layers) * LAYER + q)
    for d in range(1, LAYER):
        greet(i, layer * LAYER + lax.rem(q + d, LAYER))
    has_prev, has_next = i > 0, i < intervals - 1
    has_low, has_high = r > 0, r < rows - 1
    for there, to_i, to_r in (
        (has_prev, i - 1, r), (has_next, i + 1, r), (has_low, i, r - 1), (has_high, i, r + 1)
    ):
        pl.when(there)(lambda to_i=to_i, to_r=to_r: greet(to_i, to_r))
    neighbours = (
        has_prev.astype(jnp.int32) + has_next.astype(jnp.int32)
        + has_low.astype(jnp.int32) + has_high.astype(jnp.int32)
    )
    pl.semaphore_wait(barrier, layers - 1 + LAYER - 1 + neighbours)

    last_of_layer, first_of_layer = q == LAYER - 1, q == 0
    cross_up = jnp.logical_and(last_of_layer, has_high)
    cross_down = jnp.logical_and(first_of_layer, has_low)
    plain_up = jnp.logical_not(last_of_layer)
    plain_down = jnp.logical_not(first_of_layer)
    spare = relay_send.at[0]

    def up_plain(c):
        return remote(x.at[:, at(CHUNKS + c)], low.at[:, at(c)], up_send.at[c], low_recv.at[c], i, r + 1)

    def down_plain(c):
        return remote(x.at[:, at(c)], high.at[:, at(c)], down_send.at[c], high_recv.at[c], i, r - 1)

    def up_cross(c):
        return remote(
            x.at[:, at(CHUNKS + c)], up_a, up_send.at[c], relay_recv.at[0], i, layer * LAYER + RELAYS[c]
        )

    def down_cross(c):
        return remote(
            x.at[:, at(c)], down_a, down_send.at[c], relay_recv.at[2], i, layer * LAYER + RELAYS[c]
        )

    def onward(c):
        return remote(x.at[:, at(c)], prev.at[:, at(c)], x_send.at[c], x_recv.at[c], i + 1, r)

    @pl.when(cross_up)
    def _():
        for c in range(CHUNKS):
            up_cross(c).start()

    @pl.when(cross_down)
    def _():
        for c in range(CHUNKS):
            down_cross(c).start()

    def start_onward(first, last):
        @pl.when(has_next)
        def _():
            for c in range(first, last):
                onward(c).start()
                onward(CHUNKS + c).start()

    start_onward(0, CHUNKS // 2)

    @pl.when(plain_up)
    def _():
        for c in range(CHUNKS):
            up_plain(c).start()

    @pl.when(plain_down)
    def _():
        for c in range(CHUNKS):
            down_plain(c).start()

    acc[...] = jnp.zeros_like(acc)

    @pl.when(jnp.logical_not(has_prev))
    def _():
        prev[...] = jnp.zeros_like(prev)

    @pl.when(jnp.logical_not(has_low))
    def _():
        low[...] = jnp.zeros_like(low)

    @pl.when(jnp.logical_not(has_high))
    def _():
        high[...] = jnp.zeros_like(high)

    piece = jnp.int32(0)
    relays = q == RELAYS[0]
    for c in range(1, CHUNKS):
        piece = piece + jnp.where(q == RELAYS[c], c, 0)
        relays = jnp.logical_or(relays, q == RELAYS[c])
    above, below = layer < layers - 1, layer > 0

    def relay_steps():
        base = layer * LAYER
        return (
            (above, 0, up_a, remote(up_a, up_b, relay_send.at[0], relay_recv.at[1], i, r + LAYER)),
            (below, 2, down_a, remote(down_a, down_b, relay_send.at[2], relay_recv.at[3], i, r - LAYER)),
            (below, 1, up_b, remote(
                up_b, low.at[:, at(piece)], relay_send.at[1], low_recv.at[piece], i, base)),
            (above, 3, down_b, remote(
                down_b, high.at[:, at(piece)], relay_send.at[3], high_recv.at[piece], i, base + LAYER - 1)),
        )

    for there, slot, buffer, copy in relay_steps():
        @pl.when(jnp.logical_and(relays, there))
        def _(slot=slot, buffer=buffer, copy=copy):
            remote(buffer, buffer, spare, relay_recv.at[slot], i, r).wait_recv()
            copy.start()

    start_onward(CHUNKS // 2, CHUNKS)

    gives = lax.rem(i, 2) == 0

    def give_low(c):
        return remote(low.at[:, at(c)], plow_o.at[:, at(c)], plow_send.at[c], plow_recv.at[c], i + 1, r)

    def give_high(c):
        return remote(high.at[:, at(c)], phigh_o.at[:, at(c)], phigh_send.at[c], phigh_recv.at[c], i + 1, r)

    def writes(c):
        return (
            pltpu.make_async_copy(prev.at[:, at(c)], prev_o.at[:, at(c)], out_sem.at[0, c]),
            pltpu.make_async_copy(
                prev.at[:, at(CHUNKS + c)], prev_o.at[:, at(CHUNKS + c)], out_sem.at[1, c]),
            pltpu.make_async_copy(low.at[:, at(c)], low_o.at[:, at(c)], out_sem.at[2, c]),
            pltpu.make_async_copy(high.at[:, at(c)], high_o.at[:, at(c)], out_sem.at[3, c]),
        )

    @pl.loop(0, CHUNKS)
    def _(c):
        @pl.when(has_prev)
        def _():
            onward(c).wait_recv()
            onward(CHUNKS + c).wait_recv()

        @pl.when(has_low)
        def _():
            up_plain(c).wait_recv()

        @pl.when(has_high)
        def _():
            down_plain(c).wait_recv()

        for copy in writes(c):
            copy.start()

        @pl.when(gives)
        def _():
            give_low(c).start()
            give_high(c).start()

        for plane in range(2):
            mine = x[:, at(plane * CHUNKS + c)]
            image = stencil(x, low, high, pot, plane, c, size, width)
            theirs = prev[:, at(plane * CHUNKS + c)]
            mine_hi, mine_lo = split(mine)
            image_hi, image_lo = split(image)
            theirs_hi, theirs_lo = split(theirs)
            left = jnp.concatenate([mine_hi, theirs_hi, mine_lo, theirs_lo], axis=0)
            right = jnp.concatenate([mine_hi, image_hi, mine_lo, image_lo], axis=0)
            acc[...] += lax.dot_general(
                left, right, (((1,), (1,)), ((), ())), preferred_element_type=F32
            )

    half = acc.shape[0] // 2
    partial = acc[:half, :half] + acc[half:, half:] + (acc[:half, half:] + acc[half:, :half])

    def summed(stage, mine, place, value):
        sums[stage, mine] = value

        def copy(d):
            return remote(
                sums.at[stage, mine], sums.at[stage, mine],
                sum_send.at[stage, d], sum_recv.at[stage, mine], i, place(lax.rem(mine + d, 4)),
            )

        for d in range(1, 4):
            copy(d).start()
        for d in range(1, 4):
            theirs = lax.rem(mine + d, 4)
            remote(
                sums.at[stage, theirs], sums.at[stage, theirs],
                sum_send.at[stage, d], sum_recv.at[stage, theirs], i, r,
            ).wait_recv()
        return (sums[stage, 0] + sums[stage, 1]) + (sums[stage, 2] + sums[stage, 3])

    partial = summed(0, qy, lambda o: r - qy + o, partial)

    lone = jnp.logical_and(i > 0, lax.rem(i, 2) == 0)

    def pass_up(c):
        return remote(
            prev.at[:, at(CHUNKS + c)], plow_o.at[:, at(c)], up_send.at[c], plow_recv.at[c], i, r + 1)

    def pass_down(c):
        return remote(prev.at[:, at(c)], phigh_o.at[:, at(c)], down_send.at[c], phigh_recv.at[c], i, r - 1)

    def own_low(c):
        return pltpu.make_async_copy(low.at[:, at(c)], plow_o.at[:, at(c)], plow_recv.at[c])

    def own_high(c):
        return pltpu.make_async_copy(high.at[:, at(c)], phigh_o.at[:, at(c)], phigh_recv.at[c])

    def none_low(c):
        return pltpu.make_async_copy(prev.at[:, at(c)], plow_o.at[:, at(c)], plow_recv.at[c])

    def none_high(c):
        return pltpu.make_async_copy(prev.at[:, at(c)], phigh_o.at[:, at(c)], phigh_recv.at[c])

    @pl.when(has_high)
    def _():
        for c in range(CHUNKS):
            up_plain(c).wait_send()

    @pl.when(has_low)
    def _():
        for c in range(CHUNKS):
            down_plain(c).wait_send()

    def for_chunks(there, copies):
        @pl.when(there)
        def _():
            for c in range(CHUNKS):
                for copy in copies:
                    copy(c).start()

    for_chunks(jnp.logical_and(lone, has_high), (pass_up,))
    for_chunks(jnp.logical_and(lone, has_low), (pass_down,))
    for_chunks(jnp.logical_and(lone, jnp.logical_not(has_low)), (own_low,))
    for_chunks(jnp.logical_and(lone, jnp.logical_not(has_high)), (own_high,))
    for_chunks(jnp.logical_not(has_prev), (none_low, none_high))

    partial = summed(1, qx, lambda o: r - qx * 4 + o * 4, partial)
    partial = summed(2, layer, lambda o: o * LAYER + q, partial)
    total[...] = partial
    n = prior.shape[0]
    hand = remote(total.at[pl.ds(0, n)], prior, prior_send, prior_recv, i + 1, r)
    pl.when(has_next)(lambda: hand.start())
    pl.when(has_prev)(lambda: hand.wait_recv())

    @pl.when(jnp.logical_not(has_prev))
    def _():
        row = lax.broadcasted_iota(jnp.int32, prior.shape, 0)
        lane = lax.broadcasted_iota(jnp.int32, prior.shape, 1)
        prior[...] = jnp.where(row == lane, 1.0, 0.0)

    coefficients(total[...], prior[...], w_o, r_o)

    for c in range(CHUNKS):
        for copy in writes(c):
            copy.wait()
        give_low(c).wait_recv()
        give_high(c).wait_recv()

    @pl.when(has_next)
    def _():
        hand.wait_send()
        for c in range(2 * CHUNKS):
            onward(c).wait_send()

    @pl.when(gives)
    def _():
        for c in range(CHUNKS):
            give_low(c).wait_send()
            give_high(c).wait_send()

    @pl.when(jnp.logical_and(lone, has_high))
    def _():
        for c in range(CHUNKS):
            pass_up(c).wait_send()

    @pl.when(jnp.logical_and(lone, has_low))
    def _():
        for c in range(CHUNKS):
            pass_down(c).wait_send()

    for there, slot, buffer, copy in relay_steps():
        @pl.when(jnp.logical_and(relays, there))
        def _(copy=copy):
            copy.wait_send()

    for stage in range(3):
        for d in range(1, 4):
            remote(
                sums.at[stage, 0], sums.at[stage, 0],
                sum_send.at[stage, d], sum_recv.at[stage, 0], i, r,
            ).wait_send()


def apply_kernel(
    x_h, prev_h, low_h, high_h, plow_h, phigh_h, pot, w, basis_o, residual_o,
    x, prev, low, high, plow, phigh, out, in_sem, out_sem,
):
    size = low.shape[1]
    width = size // CHUNKS
    n = x.shape[0]

    def at(c):
        return pl.ds(pl.multiple_of(c * width, LANES), width)

    def reads(c):
        pairs = (
            (x_h, x, c), (x_h, x, CHUNKS + c), (prev_h, prev, c), (prev_h, prev, CHUNKS + c),
            (low_h, low, c), (high_h, high, c), (plow_h, plow, c), (phigh_h, phigh, c),
        )
        return [
            pltpu.make_async_copy(src.at[:, at(k)], dst.at[:, at(k)], in_sem.at[e, c])
            for e, (src, dst, k) in enumerate(pairs)
        ]

    for c in range(CHUNKS):
        for copy in reads(c):
            copy.start()

    def writes(plane, c):
        where = at(plane * CHUNKS + c)
        return [
            pltpu.make_async_copy(out.at[plane, pl.ds(e * n, n)], dst.at[:, where], out_sem.at[plane, e])
            for e, dst in enumerate((basis_o, residual_o))
        ]

    w_hi, w_lo = split(w[...])
    both = jnp.concatenate([w_hi, w_lo], axis=0)
    for copy in reads(0):
        copy.wait()

    @pl.loop(0, CHUNKS)
    def _(c):
        @pl.when(c < CHUNKS - 1)
        def _():
            for copy in reads(c + 1):
                copy.wait()

        for plane in range(2):
            k = plane * CHUNKS + c
            z = jnp.concatenate(
                [
                    x[:, at(k)],
                    prev[:, at(k)],
                    stencil(x, low, high, pot, plane, c, size, width),
                    stencil(prev, plow, phigh, pot, plane, c, size, width),
                ],
                axis=0,
            )
            z_hi, z_lo = split(z)
            wide = jnp.dot(both, z_hi, preferred_element_type=F32)
            value = (wide[: 2 * n] + wide[2 * n :]) + jnp.dot(w_hi, z_lo, preferred_element_type=F32)

            @pl.when(c > 0)
            def _():
                for copy in writes(plane, c - 1):
                    copy.wait()

            out[plane] = value
            for copy in writes(plane, c):
                copy.start()

    for plane in range(2):
        for copy in writes(plane, CHUNKS - 1):
            copy.wait()


def solution(mesh):
    intervals, rows = mesh.shape["interval"], mesh.shape["rows"]

    def body(filtered, potential):
        x = filtered[0]
        n, cells = x.shape
        size = cells // 2
        width = size // CHUNKS
        pot = potential.reshape(1, cells)
        anywhere = pl.BlockSpec(memory_space=pl.ANY)
        vmem = pl.BlockSpec(memory_space=pltpu.VMEM)
        whole = jax.ShapeDtypeStruct((n, cells), F32)
        plane = jax.ShapeDtypeStruct((n, size), F32)
        dma = pltpu.SemaphoreType.DMA

        def kernel(*refs):
            exchange_kernel(intervals, rows, *refs)

        prev, low, high, plow, phigh, w, ritz = pl.pallas_call(
            kernel,
            out_shape=(
                whole, plane, plane, plane, plane,
                jax.ShapeDtypeStruct((2 * n, 4 * n), F32),
                jax.ShapeDtypeStruct((n, n), F32),
            ),
            in_specs=[vmem, vmem],
            out_specs=(anywhere,) * 5 + (vmem, vmem),
            scratch_shapes=[
                pltpu.VMEM((n, cells), F32),
                pltpu.VMEM((n, size), F32),
                pltpu.VMEM((n, size), F32),
                *[pltpu.VMEM((n, width), F32) for _ in range(4)],
                pltpu.VMEM((4 * n, 4 * n), F32),
                pltpu.VMEM((3, 4, 2 * n, 2 * n), F32),
                pltpu.VMEM((2 * n, 2 * n), F32),
                pltpu.VMEM((n, 2 * n), F32),
                dma((2 * CHUNKS,)), dma((2 * CHUNKS,)),
                dma((CHUNKS,)), dma((CHUNKS,)), dma((CHUNKS,)), dma((CHUNKS,)),
                dma((4,)), dma((4,)),
                dma((CHUNKS,)), dma((CHUNKS,)), dma((CHUNKS,)), dma((CHUNKS,)),
                dma((4, CHUNKS)),
                dma((3, 4)), dma((3, 4)),
                dma, dma,
            ],
            compiler_params=pltpu.CompilerParams(
                collective_id=0, has_side_effects=True, vmem_limit_bytes=48 * 2**20
            ),
            name="exchange",
        )(x, pot)
        basis, residual = pl.pallas_call(
            apply_kernel,
            out_shape=(whole, whole),
            in_specs=[anywhere] * 6 + [vmem, vmem],
            out_specs=(anywhere, anywhere),
            scratch_shapes=[
                pltpu.VMEM((n, cells), F32),
                pltpu.VMEM((n, cells), F32),
                *[pltpu.VMEM((n, size), F32) for _ in range(4)],
                pltpu.VMEM((2, 2 * n, width), F32),
                dma((8, CHUNKS)), dma((2, 2)),
            ],
            compiler_params=pltpu.CompilerParams(vmem_limit_bytes=48 * 2**20),
            name="apply",
        )(x, prev, low, high, plow, phigh, pot, w)
        return basis[None], ritz[None], residual[None]

    return jax.shard_map(
        body,
        mesh=mesh,
        in_specs=(P("interval", None, "rows"), P("rows", None, None)),
        out_specs=(
            P("interval", None, "rows"),
            P("interval", None, None),
            P("interval", None, "rows"),
        ),
        check_vma=False,
    )
```

```python
import functools

import jax
import jax.numpy as jnp
from jax import lax
from jax.experimental import pallas as pl
from jax.experimental.pallas import tpu as pltpu
from jax.sharding import PartitionSpec as P

MESH = pl.DeviceIdType.MESH
F32 = jnp.float32
BF16 = jnp.bfloat16

LANES = 128
LAYER = 16
CHUNKS = 8
RELAYS = {0: 3, 1: 7, 2: 10, 5: 9, 6: 13, 7: 8}
OWN, STRAIGHT = 3, 4
FIRST_CROSS, THEN_CROSS = (6,), (0, 2, 3, 1, 7, 4, 5)
ACROSS, BESIDE = (2, 5, 7), (0, 1, 3, 4, 6)
FIRST_ONWARD, NEXT_ONWARD = 2, 4
INVERT_AT = 4


def split(v):
    hi = v.astype(BF16)
    return hi, (v - hi.astype(F32)).astype(BF16)


def exact_dot(a, b, dims):
    return lax.dot_general(
        a, b, (dims, ((), ())), precision=lax.Precision.HIGHEST, preferred_element_type=F32
    )


def stencil(u, low, high, pot, plane, j, size, width):
    base = plane * size
    start = pl.multiple_of(base + j * width, LANES)
    c = u[:, pl.ds(start, width)]
    first = pl.multiple_of(jnp.maximum(start - LANES, base), LANES)
    last = pl.multiple_of(jnp.minimum(start + width, base + size - LANES), LANES)
    before = jnp.where(j > 0, u[:, pl.ds(first, LANES)], 0.0)
    after = jnp.where(j < size // width - 1, u[:, pl.ds(last, LANES)], 0.0)
    tiles = width // LANES
    part = [c[:, t * LANES : (t + 1) * LANES] for t in range(tiles)]
    around = [before, *part, after]
    lane = lax.broadcasted_iota(jnp.int32, part[0].shape, 1)
    other = u[:, pl.ds(pl.multiple_of((1 - plane) * size + j * width, LANES), width)]
    halo = (high if plane else low)[:, pl.ds(pl.multiple_of(j * width, LANES), width)]
    weight = 6.0 + pot[:, pl.ds(start, width)]
    out = []
    for t in range(tiles):
        cut = slice(t * LANES, (t + 1) * LANES)
        left = jnp.where(lane == 0, 0.0, pltpu.roll(part[t], 1, 1))
        right = jnp.where(lane == LANES - 1, 0.0, pltpu.roll(part[t], LANES - 1, 1))
        beside = (other[:, cut] + halo[:, cut]) + (around[t] + around[t + 2]) + (left + right)
        out.append(weight[:, cut] * part[t] - beside)
    return jnp.concatenate(out, axis=1)


def inverse_factor(square):
    n = square.shape[0]
    row = lax.broadcasted_iota(jnp.int32, (n, LANES), 0)
    lane = lax.broadcasted_iota(jnp.int32, (n, LANES), 1)
    t = jnp.where(lane < n, square, jnp.where(lane == row + n, 1.0, 0.0))
    for k in range(n):
        pivot = t[k : k + 1, :]
        scaled = pivot * (1.0 / t[k : k + 1, k : k + 1])
        column = jnp.where(row > k, jnp.broadcast_to(t[:, k : k + 1], (n, LANES)), 0.0)
        t = t - column * scaled
    diagonal = jnp.sum(jnp.where(lane == row, t, 0.0), axis=1, keepdims=True)
    t = t * (1.0 / jnp.sqrt(diagonal))
    return pltpu.roll(t, LANES - n, 1)[:, :n]


def coefficients(total, inv_p, prior, wait_prior, w_out, r_out):
    n = total.shape[0] // 2
    swapped = pltpu.roll(total, n, 1)
    gram, k_own = total[:n, :n], swapped[:n, :n]
    g_pi, k_pi = total[n:, :n], swapped[n:, :n]
    et = exact_dot(inv_p, g_pi, ((1,), (0,)))
    schur = gram - exact_dot(et, et, ((0,), (0,)))
    toward = exact_dot(et, inv_p, ((0,), (0,)))
    wide = jnp.concatenate([schur, jnp.zeros_like(schur)], axis=1)
    a = inverse_factor(wide)
    b = -exact_dot(a, toward, ((1,), (0,)))
    mixed = exact_dot(b, k_pi, ((1,), (0,)))
    ritz = exact_dot(exact_dot(a, k_own, ((1,), (0,))), a, ((1,), (1,)))
    ritz = ritz + exact_dot(mixed, a, ((1,), (1,))) + exact_dot(a, mixed, ((1,), (1,)))
    wait_prior()
    k_prior = pltpu.roll(prior[...], n, 1)[:, :n]
    ritz = ritz + exact_dot(exact_dot(b, k_prior, ((1,), (0,))), b, ((1,), (1,)))
    r_out[...] = ritz
    ra = exact_dot(ritz, a, ((0,), (0,)))
    rb = exact_dot(ritz, b, ((0,), (0,)))
    zero = jnp.zeros_like(a)
    w_out[:n, :] = jnp.concatenate([a, b, zero, zero], axis=1)
    w_out[n:, :] = jnp.concatenate([-ra, -rb, a, b], axis=1)


def exchange_kernel(
    intervals, rows,
    x_h, pot,
    prev_o, low_o, high_o, plow_o, phigh_o, w_o, r_o,
    x, prev, low, high, up_a, up_b, down_a, down_b, acc, sums, total, prior, early_sums, early_total, early_prior, inv_p,
    x_send, x_recv, up_send, down_send, low_recv, high_recv,
    relay_send, relay_recv, pass_up_send, pass_down_send, plow_send, phigh_send, plow_recv, phigh_recv,
    in_sem, out_sem, sum_send, sum_recv, prior_send, prior_recv,
    early_send, early_recv, early_prior_send, early_prior_recv,
):
    i, r = lax.axis_index("interval"), lax.axis_index("rows")
    layers = rows // LAYER
    layer, q = r // LAYER, r % LAYER
    qx, qy = q // 4, q % 4
    size = low.shape[1]
    width = size // CHUNKS

    def at(c):
        return pl.ds(pl.multiple_of(c * width, LANES), width)

    def remote(src, dst, send, recv, to_i, to_r):
        return pltpu.make_async_remote_copy(
            src_ref=src, dst_ref=dst, send_sem=send, recv_sem=recv,
            device_id=(to_i, to_r), device_id_type=MESH,
        )

    loads = [
        pltpu.make_async_copy(x_h.at[:, at(c)], x.at[:, at(c)], in_sem.at[c]) for c in range(2 * CHUNKS)
    ]
    for copy in loads:
        copy.start()

    barrier = pltpu.get_barrier_semaphore()

    def greet(to_i, to_r):
        pl.semaphore_signal(barrier, inc=1, device_id=(to_i, to_r), device_id_type=MESH)

    for d in range(1, layers):
        greet(i, lax.rem(layer + d, layers) * LAYER + q)
    for d in range(1, LAYER):
        greet(i, layer * LAYER + lax.rem(q + d, LAYER))
    has_prev, has_next = i > 0, i < intervals - 1
    has_low, has_high = r > 0, r < rows - 1
    for there, to_i, to_r in (
        (has_prev, i - 1, r), (has_next, i + 1, r), (has_low, i, r - 1), (has_high, i, r + 1)
    ):
        pl.when(there)(lambda to_i=to_i, to_r=to_r: greet(to_i, to_r))
    neighbours = (
        has_prev.astype(jnp.int32) + has_next.astype(jnp.int32)
        + has_low.astype(jnp.int32) + has_high.astype(jnp.int32)
    )
    for copy in loads:
        copy.wait()
    n = prior.shape[0]
    early_acc = acc.at[pl.ds(0, 2 * n), pl.ds(0, 2 * n)]
    early_acc[...] = jnp.zeros((2 * n, 2 * n), F32)

    @pl.loop(0, 2 * CHUNKS)
    def _(c):
        both = jnp.concatenate(split(x[:, at(c)]), axis=0)
        early_acc[...] += lax.dot_general(
            both, both, (((1,), (1,)), ((), ())), preferred_element_type=F32
        )

    halves = early_acc[pl.ds(0, n), :] + pltpu.roll(early_acc[pl.ds(n, n), :], n, 1)
    own_gram = halves + pltpu.roll(halves, n, 1)
    pl.semaphore_wait(barrier, layers - 1 + LAYER - 1 + neighbours)

    places = (
        (qy, lambda o: r - qy + o), (qx, lambda o: r - qx * 4 + o * 4), (layer, lambda o: o * LAYER + q)
    )

    def sum_copy(buffer, send, recv, stage, slot, d, to_r):
        return remote(
            buffer.at[stage, slot], buffer.at[stage, slot], send.at[stage, d], recv.at[stage, slot], i, to_r)

    def sum_start(buffer, send, recv, stage, value):
        mine, place = places[stage]
        buffer[stage, mine] = value
        for d in range(1, 4):
            sum_copy(buffer, send, recv, stage, mine, d, place(lax.rem(mine + d, 4))).start()

    def sum_end(buffer, send, recv, stage):
        mine, _ = places[stage]
        for d in range(1, 4):
            sum_copy(buffer, send, recv, stage, lax.rem(mine + d, 4), d, r).wait_recv()
        return (buffer[stage, 0] + buffer[stage, 1]) + (buffer[stage, 2] + buffer[stage, 3])

    early = (early_sums, early_send, early_recv)
    late = (sums, sum_send, sum_recv)

    def summed(stage, value):
        sum_start(*late, stage, value)
        return sum_end(*late, stage)

    sum_start(*early, 0, own_gram)

    last_of_layer, first_of_layer = q == LAYER - 1, q == 0
    cross_up = jnp.logical_and(last_of_layer, has_high)
    cross_down = jnp.logical_and(first_of_layer, has_low)
    plain_up = jnp.logical_not(last_of_layer)
    plain_down = jnp.logical_not(first_of_layer)
    spare = relay_send.at[0]

    def up_plain(c):
        return remote(x.at[:, at(CHUNKS + c)], low.at[:, at(c)], up_send.at[c], low_recv.at[c], i, r + 1)

    def down_plain(c):
        return remote(x.at[:, at(c)], high.at[:, at(c)], down_send.at[c], high_recv.at[c], i, r - 1)

    base = layer * LAYER

    def up_cross(c):
        if c == STRAIGHT:
            return up_plain(c)
        dst, recv, to = (up_b, 1, r + LAYER) if c == OWN else (up_a, 0, base + RELAYS[c])
        return remote(x.at[:, at(CHUNKS + c)], dst, up_send.at[c], relay_recv.at[recv], i, to)

    def down_cross(c):
        if c == STRAIGHT:
            return down_plain(c)
        dst, recv, to = (
            (down_b, 3, r - LAYER) if c == OWN else (down_a, 2, base + LAYER - 1 - RELAYS[c])
        )
        return remote(x.at[:, at(c)], dst, down_send.at[c], relay_recv.at[recv], i, to)

    def onward(c):
        return remote(x.at[:, at(c)], prev.at[:, at(c)], x_send.at[c], x_recv.at[c], i + 1, r)

    def start_chunks(there, copies, chunks):
        @pl.when(there)
        def _():
            for c in chunks:
                for copy in copies:
                    copy(c).start()

    def onward_low(c):
        return onward(c)

    def onward_high(c):
        return onward(CHUNKS + c)

    def start_onward(first, last):
        start_chunks(has_next, (onward_low, onward_high), range(first, last))

    all_of = lambda *terms: functools.reduce(jnp.logical_and, terms)
    start_onward(0, FIRST_ONWARD)
    start_chunks(cross_up, (up_cross,), FIRST_CROSS)
    start_chunks(cross_down, (down_cross,), FIRST_CROSS)
    start_chunks(qy < 3, (up_plain,), range(CHUNKS))
    start_chunks(qy > 0, (down_plain,), range(CHUNKS))
    own_gram = sum_end(*early, 0)
    sum_start(*early, 1, own_gram)
    start_chunks(cross_up, (up_cross,), THEN_CROSS)
    start_chunks(cross_down, (down_cross,), THEN_CROSS)
    start_chunks(all_of(qy == 3, plain_up), (up_plain,), range(CHUNKS))
    start_chunks(all_of(qy == 0, plain_down), (down_plain,), range(CHUNKS))
    own_gram = sum_end(*early, 1)
    sum_start(*early, 2, own_gram)
    start_onward(FIRST_ONWARD, NEXT_ONWARD)

    acc[...] = jnp.zeros_like(acc)

    @pl.when(jnp.logical_not(has_prev))
    def _():
        prev[...] = jnp.zeros_like(prev)

    @pl.when(jnp.logical_not(has_low))
    def _():
        low[...] = jnp.zeros_like(low)

    @pl.when(jnp.logical_not(has_high))
    def _():
        high[...] = jnp.zeros_like(high)

    def role(column):
        chunk, first = jnp.int32(0), jnp.bool_(False)
        for c, of in RELAYS.items():
            chunk = chunk + jnp.where(column == of, c, 0)
            first = jnp.logical_or(first, column == of)
        own = column == LAYER - 1
        return chunk + jnp.where(own, OWN, 0), first, jnp.logical_or(first, own)

    up_chunk, up_first, up_second = role(q)
    down_chunk, down_first, down_second = role(LAYER - 1 - q)
    above, below = layer < layers - 1, layer > 0
    first_hops = (
        (jnp.logical_and(up_first, above), 0, up_a, remote(
            up_a, up_b, relay_send.at[0], relay_recv.at[1], i, r + LAYER)),
        (jnp.logical_and(down_first, below), 2, down_a, remote(
            down_a, down_b, relay_send.at[2], relay_recv.at[3], i, r - LAYER)),
    )
    second_hops = (
        (jnp.logical_and(up_second, below), 1, up_b, remote(
            up_b, low.at[:, at(up_chunk)], relay_send.at[1], low_recv.at[up_chunk], i, base)),
        (jnp.logical_and(down_second, above), 3, down_b, remote(
            down_b, high.at[:, at(down_chunk)], relay_send.at[3], high_recv.at[down_chunk],
            i, base + LAYER - 1)),
    )

    def relay(hops):
        for there, slot, buffer, copy in hops:
            @pl.when(there)
            def _(slot=slot, buffer=buffer, copy=copy):
                remote(buffer, buffer, spare, relay_recv.at[slot], i, r).wait_recv()
                copy.start()

    relay(first_hops)
    start_onward(NEXT_ONWARD, CHUNKS)
    relay(second_hops)
    early_total[...] = sum_end(*early, 2)
    early_hand = remote(early_total, early_prior, early_prior_send, early_prior_recv, i + 1, r)
    pl.when(has_next)(lambda: early_hand.start())

    @pl.when(jnp.logical_not(has_prev))
    def _():
        row = lax.broadcasted_iota(jnp.int32, early_prior.shape, 0)
        lane = lax.broadcasted_iota(jnp.int32, early_prior.shape, 1)
        early_prior[...] = jnp.where(row == lane, 1.0, 0.0)
        prior[...] = jnp.zeros_like(prior)


    gives = lax.rem(i, 2) == 0
    across = jnp.logical_and(has_next, jnp.logical_not(gives))

    def give_low(c):
        return remote(low.at[:, at(c)], plow_o.at[:, at(c)], plow_send.at[c], plow_recv.at[c], i + 1, r)

    def give_high(c):
        return remote(high.at[:, at(c)], phigh_o.at[:, at(c)], phigh_send.at[c], phigh_recv.at[c], i + 1, r)

    def writes(c):
        return (
            pltpu.make_async_copy(prev.at[:, at(c)], prev_o.at[:, at(c)], out_sem.at[0, c]),
            pltpu.make_async_copy(
                prev.at[:, at(CHUNKS + c)], prev_o.at[:, at(CHUNKS + c)], out_sem.at[1, c]),
            pltpu.make_async_copy(low.at[:, at(c)], low_o.at[:, at(c)], out_sem.at[2, c]),
            pltpu.make_async_copy(high.at[:, at(c)], high_o.at[:, at(c)], out_sem.at[3, c]),
        )

    lone = jnp.logical_and(has_prev, gives)

    def invert():
        pl.when(has_prev)(lambda: early_hand.wait_recv())
        inv_p[...] = inverse_factor(early_prior[...])

    @pl.loop(0, CHUNKS)
    def _(c):
        pl.when(jnp.logical_and(c == INVERT_AT, jnp.logical_not(lone)))(invert)

        @pl.when(has_prev)
        def _():
            onward(c).wait_recv()
            onward(CHUNKS + c).wait_recv()

        @pl.when(has_low)
        def _():
            up_plain(c).wait_recv()

        @pl.when(has_high)
        def _():
            down_plain(c).wait_recv()

        for copy in writes(c):
            copy.start()

        @pl.when(gives)
        def _():
            give_low(c).start()
            give_high(c).start()

        for plane in range(2):
            mine = x[:, at(plane * CHUNKS + c)]
            image = stencil(x, low, high, pot, plane, c, size, width)
            theirs = prev[:, at(plane * CHUNKS + c)]
            mine_hi, mine_lo = split(mine)
            image_hi, image_lo = split(image)
            theirs_hi, theirs_lo = split(theirs)
            left = jnp.concatenate([mine_hi, theirs_hi, mine_lo, theirs_lo], axis=0)
            right = jnp.concatenate([mine_hi, image_hi, mine_lo, image_lo], axis=0)
            acc[...] += lax.dot_general(
                left, right, (((1,), (1,)), ((), ())), preferred_element_type=F32
            )

    half = acc.shape[0] // 2
    partial = acc[:half, :half] + acc[half:, half:] + (acc[:half, half:] + acc[half:, :half])

    def pass_up(c):
        return remote(
            prev.at[:, at(CHUNKS + c)], plow_o.at[:, at(c)], pass_up_send.at[c], plow_recv.at[c], i, r + 1)

    def pass_down(c):
        return remote(
            prev.at[:, at(c)], phigh_o.at[:, at(c)], pass_down_send.at[c], phigh_recv.at[c], i, r - 1)

    def none_low(c):
        return pltpu.make_async_copy(prev.at[:, at(c)], plow_o.at[:, at(c)], plow_recv.at[c])

    def none_high(c):
        return pltpu.make_async_copy(prev.at[:, at(c)], phigh_o.at[:, at(c)], phigh_recv.at[c])

    def own_low(c):
        return pltpu.make_async_copy(low.at[:, at(c)], plow_o.at[:, at(c)], plow_recv.at[c])

    def own_high(c):
        return pltpu.make_async_copy(high.at[:, at(c)], phigh_o.at[:, at(c)], phigh_recv.at[c])

    start_chunks(jnp.logical_not(has_prev), (none_low, none_high), range(CHUNKS))
    start_chunks(all_of(lone, jnp.logical_not(has_low)), (own_low,), BESIDE)
    start_chunks(all_of(lone, jnp.logical_not(has_high)), (own_high,), BESIDE)
    sum_start(*late, 0, partial)
    pl.when(lone)(invert)
    partial = sum_end(*late, 0)
    partial = summed(1, partial)
    partial = summed(2, partial)
    total[...] = partial
    hand = remote(total.at[pl.ds(0, n)], prior, prior_send, prior_recv, i + 1, r)
    pl.when(has_next)(lambda: hand.start())
    start_chunks(all_of(lone, has_high), (pass_up,), BESIDE)
    start_chunks(all_of(lone, has_low), (pass_down,), BESIDE)
    start_chunks(across, (give_low, give_high), ACROSS)
    wait_prior = lambda: pl.when(has_prev)(lambda: hand.wait_recv())
    coefficients(total[...], inv_p[...], prior, wait_prior, w_o, r_o)

    for c in range(CHUNKS):
        for copy in writes(c):
            copy.wait()
        give_low(c).wait_recv()
        give_high(c).wait_recv()

    def end_chunks(there, copies, chunks):
        @pl.when(there)
        def _():
            for c in chunks:
                for copy in copies:
                    copy(c).wait_send()

    end_chunks(has_high, (up_plain,), range(CHUNKS))
    end_chunks(has_low, (down_plain,), range(CHUNKS))
    pl.when(has_next)(lambda: hand.wait_send())
    pl.when(has_next)(lambda: early_hand.wait_send())
    end_chunks(has_next, (onward,), range(2 * CHUNKS))
    end_chunks(gives, (give_low, give_high), range(CHUNKS))
    end_chunks(across, (give_low, give_high), ACROSS)
    end_chunks(all_of(lone, has_high), (pass_up,), BESIDE)
    end_chunks(all_of(lone, has_low), (pass_down,), BESIDE)
    for there, _, _, copy in first_hops + second_hops:
        pl.when(there)(lambda copy=copy: copy.wait_send())

    for stage in range(3):
        for d in range(1, 4):
            sum_copy(*early, stage, 0, d, r).wait_send()
            sum_copy(*late, stage, 0, d, r).wait_send()


def apply_kernel(
    x_h, prev_h, low_h, high_h, plow_h, phigh_h, pot, w, basis_o, residual_o,
    x, prev, low, high, plow, phigh, out, in_sem, out_sem,
):
    size = low.shape[1]
    width = size // CHUNKS
    n = x.shape[0]

    def at(c):
        return pl.ds(pl.multiple_of(c * width, LANES), width)

    def reads(c):
        pairs = (
            (x_h, x, c), (x_h, x, CHUNKS + c), (prev_h, prev, c), (prev_h, prev, CHUNKS + c),
            (low_h, low, c), (high_h, high, c), (plow_h, plow, c), (phigh_h, phigh, c),
        )
        return [
            pltpu.make_async_copy(src.at[:, at(k)], dst.at[:, at(k)], in_sem.at[e, c])
            for e, (src, dst, k) in enumerate(pairs)
        ]

    for c in range(CHUNKS):
        for copy in reads(c):
            copy.start()

    def writes(plane, c):
        where = at(plane * CHUNKS + c)
        return [
            pltpu.make_async_copy(out.at[plane, pl.ds(e * n, n)], dst.at[:, where], out_sem.at[plane, e])
            for e, dst in enumerate((basis_o, residual_o))
        ]

    w_hi, w_lo = split(w[...])
    both = jnp.concatenate([w_hi, w_lo], axis=0)
    for copy in reads(0):
        copy.wait()

    @pl.loop(0, CHUNKS)
    def _(c):
        @pl.when(c < CHUNKS - 1)
        def _():
            for copy in reads(c + 1):
                copy.wait()

        for plane in range(2):
            k = plane * CHUNKS + c
            z = jnp.concatenate(
                [
                    x[:, at(k)],
                    prev[:, at(k)],
                    stencil(x, low, high, pot, plane, c, size, width),
                    stencil(prev, plow, phigh, pot, plane, c, size, width),
                ],
                axis=0,
            )
            z_hi, z_lo = split(z)
            wide = jnp.dot(both, z_hi, preferred_element_type=F32)
            value = (wide[: 2 * n] + wide[2 * n :]) + jnp.dot(w_hi, z_lo, preferred_element_type=F32)

            @pl.when(c > 0)
            def _():
                for copy in writes(plane, c - 1):
                    copy.wait()

            out[plane] = value
            for copy in writes(plane, c):
                copy.start()

    for plane in range(2):
        for copy in writes(plane, CHUNKS - 1):
            copy.wait()


def solution(mesh):
    intervals, rows = mesh.shape["interval"], mesh.shape["rows"]

    def body(filtered, potential):
        x = filtered[0]
        n, cells = x.shape
        size = cells // 2
        width = size // CHUNKS
        pot = potential.reshape(1, cells)
        anywhere = pl.BlockSpec(memory_space=pl.ANY)
        vmem = pl.BlockSpec(memory_space=pltpu.VMEM)
        whole = jax.ShapeDtypeStruct((n, cells), F32)
        plane = jax.ShapeDtypeStruct((n, size), F32)
        dma = pltpu.SemaphoreType.DMA

        def kernel(*refs):
            exchange_kernel(intervals, rows, *refs)

        prev, low, high, plow, phigh, w, ritz = pl.pallas_call(
            kernel,
            out_shape=(
                whole, plane, plane, plane, plane,
                jax.ShapeDtypeStruct((2 * n, 4 * n), F32),
                jax.ShapeDtypeStruct((n, n), F32),
            ),
            in_specs=[anywhere, vmem],
            out_specs=(anywhere,) * 5 + (vmem, vmem),
            scratch_shapes=[
                pltpu.VMEM((n, cells), F32),
                pltpu.VMEM((n, cells), F32),
                pltpu.VMEM((n, size), F32),
                pltpu.VMEM((n, size), F32),
                *[pltpu.VMEM((n, width), F32) for _ in range(4)],
                pltpu.VMEM((4 * n, 4 * n), F32),
                pltpu.VMEM((3, 4, 2 * n, 2 * n), F32),
                pltpu.VMEM((2 * n, 2 * n), F32),
                pltpu.VMEM((n, 2 * n), F32),
                pltpu.VMEM((3, 4, n, 2 * n), F32),
                pltpu.VMEM((n, 2 * n), F32),
                pltpu.VMEM((n, 2 * n), F32),
                pltpu.VMEM((n, n), F32),
                dma((2 * CHUNKS,)), dma((2 * CHUNKS,)),
                dma((CHUNKS,)), dma((CHUNKS,)), dma((CHUNKS,)), dma((CHUNKS,)),
                dma((4,)), dma((4,)),
                dma((CHUNKS,)), dma((CHUNKS,)),
                dma((CHUNKS,)), dma((CHUNKS,)), dma((CHUNKS,)), dma((CHUNKS,)),
                dma((2 * CHUNKS,)), dma((4, CHUNKS)),
                dma((3, 4)), dma((3, 4)),
                dma, dma,
                dma((3, 4)), dma((3, 4)),
                dma, dma,
            ],
            compiler_params=pltpu.CompilerParams(
                collective_id=0, has_side_effects=True, vmem_limit_bytes=48 * 2**20
            ),
            name="exchange",
        )(x, pot)
        basis, residual = pl.pallas_call(
            apply_kernel,
            out_shape=(whole, whole),
            in_specs=[anywhere] * 6 + [vmem, vmem],
            out_specs=(anywhere, anywhere),
            scratch_shapes=[
                pltpu.VMEM((n, cells), F32),
                pltpu.VMEM((n, cells), F32),
                *[pltpu.VMEM((n, size), F32) for _ in range(4)],
                pltpu.VMEM((2, 2 * n, width), F32),
                dma((8, CHUNKS)), dma((2, 2)),
            ],
            compiler_params=pltpu.CompilerParams(vmem_limit_bytes=48 * 2**20),
            name="apply",
        )(x, prev, low, high, plow, phigh, pot, w)
        return basis[None], ritz[None], residual[None]

    return jax.shard_map(
        body,
        mesh=mesh,
        in_specs=(P("interval", None, "rows"), P("rows", None, None)),
        out_specs=(
            P("interval", None, "rows"),
            P("interval", None, None),
            P("interval", None, "rows"),
        ),
        check_vma=False,
    )
```

```python
import functools

import jax
import jax.numpy as jnp
from jax import lax
from jax.experimental import pallas as pl
from jax.experimental.pallas import tpu as pltpu
from jax.sharding import PartitionSpec as P

MESH = pl.DeviceIdType.MESH
F32 = jnp.float32
BF16 = jnp.bfloat16

LANES = 128
LAYER = 16
CHUNKS = 8
RELAYS = {0: 3, 1: 7, 2: 10, 5: 14, 6: 13, 7: 8}
LANDING = 4
FIRST_CROSS, THEN_CROSS = (6, 5), (4, 2, 0, 1, 3, 7)
ACROSS, BESIDE = (2, 5, 7), (0, 1, 3, 4, 6)
FIRST_ONWARD, NEXT_ONWARD = 2, 4
INVERT_AT = 5


def split(v):
    hi = v.astype(BF16)
    return hi, (v - hi.astype(F32)).astype(BF16)


def exact_dot(a, b, dims):
    return lax.dot_general(
        a, b, (dims, ((), ())), precision=lax.Precision.HIGHEST, preferred_element_type=F32
    )


def stencil(u, low, high, pot, plane, j, size, width):
    base = plane * size
    start = pl.multiple_of(base + j * width, LANES)
    c = u[:, pl.ds(start, width)]
    first = pl.multiple_of(jnp.maximum(start - LANES, base), LANES)
    last = pl.multiple_of(jnp.minimum(start + width, base + size - LANES), LANES)
    before = jnp.where(j > 0, u[:, pl.ds(first, LANES)], 0.0)
    after = jnp.where(j < size // width - 1, u[:, pl.ds(last, LANES)], 0.0)
    tiles = width // LANES
    part = [c[:, t * LANES : (t + 1) * LANES] for t in range(tiles)]
    around = [before, *part, after]
    lane = lax.broadcasted_iota(jnp.int32, part[0].shape, 1)
    other = u[:, pl.ds(pl.multiple_of((1 - plane) * size + j * width, LANES), width)]
    halo = (high if plane else low)[:, pl.ds(pl.multiple_of(j * width, LANES), width)]
    weight = 6.0 + pot[:, pl.ds(start, width)]
    out = []
    for t in range(tiles):
        cut = slice(t * LANES, (t + 1) * LANES)
        left = jnp.where(lane == 0, 0.0, pltpu.roll(part[t], 1, 1))
        right = jnp.where(lane == LANES - 1, 0.0, pltpu.roll(part[t], LANES - 1, 1))
        beside = (other[:, cut] + halo[:, cut]) + (around[t] + around[t + 2]) + (left + right)
        out.append(weight[:, cut] * part[t] - beside)
    return jnp.concatenate(out, axis=1)


def inverse_factor(square):
    n = square.shape[0]
    row = lax.broadcasted_iota(jnp.int32, (n, LANES), 0)
    lane = lax.broadcasted_iota(jnp.int32, (n, LANES), 1)
    t = jnp.where(lane < n, square, jnp.where(lane == row + n, 1.0, 0.0))
    for k in range(n):
        pivot = t[k : k + 1, :]
        scaled = pivot * (1.0 / t[k : k + 1, k : k + 1])
        column = jnp.where(row > k, jnp.broadcast_to(t[:, k : k + 1], (n, LANES)), 0.0)
        t = t - column * scaled
    diagonal = jnp.sum(jnp.where(lane == row, t, 0.0), axis=1, keepdims=True)
    t = t * (1.0 / jnp.sqrt(diagonal))
    return pltpu.roll(t, LANES - n, 1)[:, :n]


def coefficients(total, inv_p, prior, wait_prior, w_out, r_out):
    n = total.shape[0] // 2
    swapped = pltpu.roll(total, n, 1)
    gram, k_own = total[:n, :n], swapped[:n, :n]
    g_pi, k_pi = total[n:, :n], swapped[n:, :n]
    et = exact_dot(inv_p, g_pi, ((1,), (0,)))
    schur = gram - exact_dot(et, et, ((0,), (0,)))
    toward = exact_dot(et, inv_p, ((0,), (0,)))
    wide = jnp.concatenate([schur, jnp.zeros_like(schur)], axis=1)
    a = inverse_factor(wide)
    b = -exact_dot(a, toward, ((1,), (0,)))
    mixed = exact_dot(b, k_pi, ((1,), (0,)))
    ritz = exact_dot(exact_dot(a, k_own, ((1,), (0,))), a, ((1,), (1,)))
    ritz = ritz + exact_dot(mixed, a, ((1,), (1,))) + exact_dot(a, mixed, ((1,), (1,)))
    wait_prior()
    k_prior = pltpu.roll(prior[...], n, 1)[:, :n]
    ritz = ritz + exact_dot(exact_dot(b, k_prior, ((1,), (0,))), b, ((1,), (1,)))
    r_out[...] = ritz
    ra = exact_dot(ritz, a, ((0,), (0,)))
    rb = exact_dot(ritz, b, ((0,), (0,)))
    zero = jnp.zeros_like(a)
    w_out[:n, :] = jnp.concatenate([a, b, zero, zero], axis=1)
    w_out[n:, :] = jnp.concatenate([-ra, -rb, a, b], axis=1)


def exchange_kernel(
    intervals, rows,
    x_h, pot,
    prev_o, low_o, high_o, plow_o, phigh_o, w_o, r_o,
    x, prev, low, high, up_a, up_b, down_a, down_b, acc, sums, total, prior, early_sums, early_total, early_prior, inv_p,
    x_send, x_recv, up_send, down_send, low_recv, high_recv,
    relay_send, relay_recv, pass_up_send, pass_down_send, plow_send, phigh_send, plow_recv, phigh_recv,
    in_sem, out_sem, sum_send, sum_recv, prior_send, prior_recv,
    early_send, early_recv, early_prior_send, early_prior_recv,
):
    i, r = lax.axis_index("interval"), lax.axis_index("rows")
    layers = rows // LAYER
    layer, q = r // LAYER, r % LAYER
    qx, qy = q // 4, q % 4
    size = low.shape[1]
    width = size // CHUNKS

    def at(c):
        return pl.ds(pl.multiple_of(c * width, LANES), width)

    def remote(src, dst, send, recv, to_i, to_r):
        return pltpu.make_async_remote_copy(
            src_ref=src, dst_ref=dst, send_sem=send, recv_sem=recv,
            device_id=(to_i, to_r), device_id_type=MESH,
        )

    loads = [
        pltpu.make_async_copy(x_h.at[:, at(c)], x.at[:, at(c)], in_sem.at[c]) for c in range(2 * CHUNKS)
    ]
    for copy in loads:
        copy.start()

    barrier = pltpu.get_barrier_semaphore()

    def greet(to_i, to_r):
        pl.semaphore_signal(barrier, inc=1, device_id=(to_i, to_r), device_id_type=MESH)

    for d in range(1, layers):
        greet(i, lax.rem(layer + d, layers) * LAYER + q)
    for d in range(1, LAYER):
        greet(i, layer * LAYER + lax.rem(q + d, LAYER))
    has_prev, has_next = i > 0, i < intervals - 1
    has_low, has_high = r > 0, r < rows - 1
    for there, to_i, to_r in (
        (has_prev, i - 1, r), (has_next, i + 1, r), (has_low, i, r - 1), (has_high, i, r + 1)
    ):
        pl.when(there)(lambda to_i=to_i, to_r=to_r: greet(to_i, to_r))
    neighbours = (
        has_prev.astype(jnp.int32) + has_next.astype(jnp.int32)
        + has_low.astype(jnp.int32) + has_high.astype(jnp.int32)
    )
    for copy in loads:
        copy.wait()
    n = prior.shape[0]
    early_acc = acc.at[pl.ds(0, 2 * n), pl.ds(0, 2 * n)]
    early_acc[...] = jnp.zeros((2 * n, 2 * n), F32)

    @pl.loop(0, 2 * CHUNKS)
    def _(c):
        both = jnp.concatenate(split(x[:, at(c)]), axis=0)
        early_acc[...] += lax.dot_general(
            both, both, (((1,), (1,)), ((), ())), preferred_element_type=F32
        )

    halves = early_acc[pl.ds(0, n), :] + pltpu.roll(early_acc[pl.ds(n, n), :], n, 1)
    own_gram = halves + pltpu.roll(halves, n, 1)
    pl.semaphore_wait(barrier, layers - 1 + LAYER - 1 + neighbours)

    places = (
        (qy, lambda o: r - qy + o), (qx, lambda o: r - qx * 4 + o * 4), (layer, lambda o: o * LAYER + q)
    )

    def sum_copy(buffer, send, recv, stage, slot, d, to_r):
        return remote(
            buffer.at[stage, slot], buffer.at[stage, slot], send.at[stage, d], recv.at[stage, slot], i, to_r)

    def sum_start(buffer, send, recv, stage, value):
        mine, place = places[stage]
        buffer[stage, mine] = value
        for d in range(1, 4):
            sum_copy(buffer, send, recv, stage, mine, d, place(lax.rem(mine + d, 4))).start()

    def sum_end(buffer, send, recv, stage):
        mine, _ = places[stage]
        for d in range(1, 4):
            sum_copy(buffer, send, recv, stage, lax.rem(mine + d, 4), d, r).wait_recv()
        return (buffer[stage, 0] + buffer[stage, 1]) + (buffer[stage, 2] + buffer[stage, 3])

    early = (early_sums, early_send, early_recv)
    late = (sums, sum_send, sum_recv)

    def summed(stage, value):
        sum_start(*late, stage, value)
        return sum_end(*late, stage)

    sum_start(*early, 0, own_gram)

    last_of_layer, first_of_layer = q == LAYER - 1, q == 0
    cross_up = jnp.logical_and(last_of_layer, has_high)
    cross_down = jnp.logical_and(first_of_layer, has_low)
    plain_up = jnp.logical_not(last_of_layer)
    plain_down = jnp.logical_not(first_of_layer)
    spare = relay_send.at[0]

    def up_plain(c):
        return remote(x.at[:, at(CHUNKS + c)], low.at[:, at(c)], up_send.at[c], low_recv.at[c], i, r + 1)

    def down_plain(c):
        return remote(x.at[:, at(c)], high.at[:, at(c)], down_send.at[c], high_recv.at[c], i, r - 1)

    base = layer * LAYER

    def up_cross(c):
        if c not in RELAYS and c != LANDING:
            return up_plain(c)
        return remote(
            x.at[:, at(CHUNKS + c)], up_a, up_send.at[c], relay_recv.at[0], i, base + RELAYS.get(c, 0))

    def down_cross(c):
        if c not in RELAYS and c != LANDING:
            return down_plain(c)
        return remote(
            x.at[:, at(c)], down_a, down_send.at[c], relay_recv.at[2],
            i, base + LAYER - 1 - RELAYS.get(c, 0))

    def onward(c):
        return remote(x.at[:, at(c)], prev.at[:, at(c)], x_send.at[c], x_recv.at[c], i + 1, r)

    def start_chunks(there, copies, chunks):
        @pl.when(there)
        def _():
            for c in chunks:
                for copy in copies:
                    copy(c).start()

    def onward_low(c):
        return onward(c)

    def onward_high(c):
        return onward(CHUNKS + c)

    def start_onward(first, last):
        start_chunks(has_next, (onward_low, onward_high), range(first, last))

    all_of = lambda *terms: functools.reduce(jnp.logical_and, terms)
    start_onward(0, FIRST_ONWARD)
    start_chunks(cross_up, (up_cross,), FIRST_CROSS)
    start_chunks(cross_down, (down_cross,), FIRST_CROSS)
    start_chunks(qy < 3, (up_plain,), range(CHUNKS))
    start_chunks(qy > 0, (down_plain,), range(CHUNKS))
    own_gram = sum_end(*early, 0)
    sum_start(*early, 1, own_gram)
    start_chunks(cross_up, (up_cross,), THEN_CROSS)
    start_chunks(cross_down, (down_cross,), THEN_CROSS)
    start_chunks(all_of(qy == 3, plain_up), (up_plain,), range(CHUNKS))
    start_chunks(all_of(qy == 0, plain_down), (down_plain,), range(CHUNKS))
    own_gram = sum_end(*early, 1)
    sum_start(*early, 2, own_gram)
    start_onward(FIRST_ONWARD, NEXT_ONWARD)

    acc[...] = jnp.zeros_like(acc)

    @pl.when(jnp.logical_not(has_prev))
    def _():
        prev[...] = jnp.zeros_like(prev)

    @pl.when(jnp.logical_not(has_low))
    def _():
        low[...] = jnp.zeros_like(low)

    @pl.when(jnp.logical_not(has_high))
    def _():
        high[...] = jnp.zeros_like(high)

    def role(column):
        chunk, first = jnp.int32(0), jnp.bool_(False)
        for c, of in RELAYS.items():
            chunk = chunk + jnp.where(column == of, c, 0)
            first = jnp.logical_or(first, column == of)
        return chunk, first

    up_chunk, up_relay = role(q)
    down_chunk, down_relay = role(LAYER - 1 - q)
    above, below = layer < layers - 1, layer > 0
    first_hops = (
        (jnp.logical_and(up_relay, above), 0, up_a, remote(
            up_a, up_b, relay_send.at[0], relay_recv.at[1], i, r + LAYER)),
        (jnp.logical_and(down_relay, below), 2, down_a, remote(
            down_a, down_b, relay_send.at[2], relay_recv.at[3], i, r - LAYER)),
        (jnp.logical_and(first_of_layer, above), 0, up_a, remote(
            up_a, low.at[:, at(LANDING)], relay_send.at[0], low_recv.at[LANDING], i, r + LAYER)),
        (jnp.logical_and(last_of_layer, below), 2, down_a, remote(
            down_a, high.at[:, at(LANDING)], relay_send.at[2], high_recv.at[LANDING], i, r - LAYER)),
    )
    second_hops = (
        (jnp.logical_and(up_relay, below), 1, up_b, remote(
            up_b, low.at[:, at(up_chunk)], relay_send.at[1], low_recv.at[up_chunk], i, base)),
        (jnp.logical_and(down_relay, above), 3, down_b, remote(
            down_b, high.at[:, at(down_chunk)], relay_send.at[3], high_recv.at[down_chunk],
            i, base + LAYER - 1)),
    )

    def relay(hops):
        for there, slot, buffer, copy in hops:
            @pl.when(there)
            def _(slot=slot, buffer=buffer, copy=copy):
                remote(buffer, buffer, spare, relay_recv.at[slot], i, r).wait_recv()
                copy.start()

    relay(first_hops)
    start_onward(NEXT_ONWARD, CHUNKS)
    relay(second_hops)
    early_total[...] = sum_end(*early, 2)
    early_hand = remote(early_total, early_prior, early_prior_send, early_prior_recv, i + 1, r)
    pl.when(has_next)(lambda: early_hand.start())

    @pl.when(jnp.logical_not(has_prev))
    def _():
        row = lax.broadcasted_iota(jnp.int32, early_prior.shape, 0)
        lane = lax.broadcasted_iota(jnp.int32, early_prior.shape, 1)
        early_prior[...] = jnp.where(row == lane, 1.0, 0.0)
        prior[...] = jnp.zeros_like(prior)


    gives = lax.rem(i, 2) == 0
    across = jnp.logical_and(has_next, jnp.logical_not(gives))

    def give_low(c):
        return remote(low.at[:, at(c)], plow_o.at[:, at(c)], plow_send.at[c], plow_recv.at[c], i + 1, r)

    def give_high(c):
        return remote(high.at[:, at(c)], phigh_o.at[:, at(c)], phigh_send.at[c], phigh_recv.at[c], i + 1, r)

    def writes(c):
        return (
            pltpu.make_async_copy(prev.at[:, at(c)], prev_o.at[:, at(c)], out_sem.at[0, c]),
            pltpu.make_async_copy(
                prev.at[:, at(CHUNKS + c)], prev_o.at[:, at(CHUNKS + c)], out_sem.at[1, c]),
            pltpu.make_async_copy(low.at[:, at(c)], low_o.at[:, at(c)], out_sem.at[2, c]),
            pltpu.make_async_copy(high.at[:, at(c)], high_o.at[:, at(c)], out_sem.at[3, c]),
        )

    lone = jnp.logical_and(has_prev, gives)

    def invert():
        pl.when(has_prev)(lambda: early_hand.wait_recv())
        inv_p[...] = inverse_factor(early_prior[...])

    @pl.loop(0, CHUNKS)
    def _(c):
        pl.when(jnp.logical_and(c == INVERT_AT, jnp.logical_not(lone)))(invert)

        @pl.when(has_prev)
        def _():
            onward(c).wait_recv()
            onward(CHUNKS + c).wait_recv()

        @pl.when(has_low)
        def _():
            up_plain(c).wait_recv()

        @pl.when(has_high)
        def _():
            down_plain(c).wait_recv()

        for copy in writes(c):
            copy.start()

        @pl.when(gives)
        def _():
            give_low(c).start()
            give_high(c).start()

        for plane in range(2):
            mine = x[:, at(plane * CHUNKS + c)]
            image = stencil(x, low, high, pot, plane, c, size, width)
            theirs = prev[:, at(plane * CHUNKS + c)]
            mine_hi, mine_lo = split(mine)
            image_hi, image_lo = split(image)
            theirs_hi, theirs_lo = split(theirs)
            left = jnp.concatenate([mine_hi, theirs_hi, mine_lo, theirs_lo], axis=0)
            right = jnp.concatenate([mine_hi, image_hi, mine_lo, image_lo], axis=0)
            acc[...] += lax.dot_general(
                left, right, (((1,), (1,)), ((), ())), preferred_element_type=F32
            )

    half = acc.shape[0] // 2
    partial = acc[:half, :half] + acc[half:, half:] + (acc[:half, half:] + acc[half:, :half])

    def pass_up(c):
        return remote(
            prev.at[:, at(CHUNKS + c)], plow_o.at[:, at(c)], pass_up_send.at[c], plow_recv.at[c], i, r + 1)

    def pass_down(c):
        return remote(
            prev.at[:, at(c)], phigh_o.at[:, at(c)], pass_down_send.at[c], phigh_recv.at[c], i, r - 1)

    def none_low(c):
        return pltpu.make_async_copy(prev.at[:, at(c)], plow_o.at[:, at(c)], plow_recv.at[c])

    def none_high(c):
        return pltpu.make_async_copy(prev.at[:, at(c)], phigh_o.at[:, at(c)], phigh_recv.at[c])

    def own_low(c):
        return pltpu.make_async_copy(low.at[:, at(c)], plow_o.at[:, at(c)], plow_recv.at[c])

    def own_high(c):
        return pltpu.make_async_copy(high.at[:, at(c)], phigh_o.at[:, at(c)], phigh_recv.at[c])

    start_chunks(jnp.logical_not(has_prev), (none_low, none_high), range(CHUNKS))
    start_chunks(all_of(lone, jnp.logical_not(has_low)), (own_low,), BESIDE)
    start_chunks(all_of(lone, jnp.logical_not(has_high)), (own_high,), BESIDE)
    passes = (
        (all_of(lone, qy < 3), pass_up, BESIDE),
        (all_of(lone, q == LAYER - 2, above), pass_up, ACROSS),
        (all_of(lone, qy > 0), pass_down, BESIDE),
        (all_of(lone, q == 1, below), pass_down, ACROSS),
        (all_of(lone, qy == 3, plain_up), pass_up, BESIDE),
        (all_of(lone, qy == 0, plain_down), pass_down, BESIDE),
    )
    only_high, only_low = jnp.logical_and(across, cross_up), jnp.logical_and(across, cross_down)
    not_up = jnp.logical_and(across, jnp.logical_not(cross_up))
    not_down = jnp.logical_and(across, jnp.logical_not(cross_down))

    sum_start(*late, 0, partial)
    for there, copy, chunks in passes[:4]:
        start_chunks(there, (copy,), chunks)
    pl.when(lone)(invert)
    partial = sum_end(*late, 0)
    partial = summed(1, partial)
    for there, copy, chunks in passes[4:]:
        start_chunks(there, (copy,), chunks)
    sum_start(*late, 2, partial)
    start_chunks(not_up, (give_low,), ACROSS[:1])
    start_chunks(not_down, (give_high,), ACROSS[:1])
    total[...] = sum_end(*late, 2)
    hand = remote(total.at[pl.ds(0, n)], prior, prior_send, prior_recv, i + 1, r)
    pl.when(has_next)(lambda: hand.start())
    start_chunks(not_up, (give_low,), ACROSS[1:])
    start_chunks(not_down, (give_high,), ACROSS[1:])
    start_chunks(only_low, (give_low,), BESIDE)
    start_chunks(only_high, (give_high,), BESIDE)
    wait_prior = lambda: pl.when(has_prev)(lambda: hand.wait_recv())
    coefficients(total[...], inv_p[...], prior, wait_prior, w_o, r_o)

    for c in range(CHUNKS):
        for copy in writes(c):
            copy.wait()
        give_low(c).wait_recv()
        give_high(c).wait_recv()

    def end_chunks(there, copies, chunks):
        @pl.when(there)
        def _():
            for c in chunks:
                for copy in copies:
                    copy(c).wait_send()

    end_chunks(has_high, (up_plain,), range(CHUNKS))
    end_chunks(has_low, (down_plain,), range(CHUNKS))
    pl.when(has_next)(lambda: hand.wait_send())
    pl.when(has_next)(lambda: early_hand.wait_send())
    end_chunks(has_next, (onward,), range(2 * CHUNKS))
    end_chunks(gives, (give_low, give_high), range(CHUNKS))
    end_chunks(not_up, (give_low,), ACROSS)
    end_chunks(not_down, (give_high,), ACROSS)
    end_chunks(only_low, (give_low,), BESIDE)
    end_chunks(only_high, (give_high,), BESIDE)
    for there, copy, chunks in passes:
        end_chunks(there, (copy,), chunks)
    for there, _, _, copy in first_hops + second_hops:
        pl.when(there)(lambda copy=copy: copy.wait_send())

    for stage in range(3):
        for d in range(1, 4):
            sum_copy(*early, stage, 0, d, r).wait_send()
            sum_copy(*late, stage, 0, d, r).wait_send()


def apply_kernel(
    x_h, prev_h, low_h, high_h, plow_h, phigh_h, pot, w, basis_o, residual_o,
    x, prev, low, high, plow, phigh, out, in_sem, out_sem,
):
    size = low.shape[1]
    width = size // CHUNKS
    n = x.shape[0]

    def at(c):
        return pl.ds(pl.multiple_of(c * width, LANES), width)

    def reads(c):
        pairs = (
            (x_h, x, c), (x_h, x, CHUNKS + c), (prev_h, prev, c), (prev_h, prev, CHUNKS + c),
            (low_h, low, c), (high_h, high, c), (plow_h, plow, c), (phigh_h, phigh, c),
        )
        return [
            pltpu.make_async_copy(src.at[:, at(k)], dst.at[:, at(k)], in_sem.at[e, c])
            for e, (src, dst, k) in enumerate(pairs)
        ]

    for c in range(CHUNKS):
        for copy in reads(c):
            copy.start()

    def writes(plane, c):
        where = at(plane * CHUNKS + c)
        return [
            pltpu.make_async_copy(out.at[plane, pl.ds(e * n, n)], dst.at[:, where], out_sem.at[plane, e])
            for e, dst in enumerate((basis_o, residual_o))
        ]

    w_hi, w_lo = split(w[...])
    both = jnp.concatenate([w_hi, w_lo], axis=0)
    for copy in reads(0):
        copy.wait()

    @pl.loop(0, CHUNKS)
    def _(c):
        @pl.when(c < CHUNKS - 1)
        def _():
            for copy in reads(c + 1):
                copy.wait()

        for plane in range(2):
            k = plane * CHUNKS + c
            z = jnp.concatenate(
                [
                    x[:, at(k)],
                    prev[:, at(k)],
                    stencil(x, low, high, pot, plane, c, size, width),
                    stencil(prev, plow, phigh, pot, plane, c, size, width),
                ],
                axis=0,
            )
            z_hi, z_lo = split(z)
            wide = jnp.dot(both, z_hi, preferred_element_type=F32)
            value = (wide[: 2 * n] + wide[2 * n :]) + jnp.dot(w_hi, z_lo, preferred_element_type=F32)

            @pl.when(c > 0)
            def _():
                for copy in writes(plane, c - 1):
                    copy.wait()

            out[plane] = value
            for copy in writes(plane, c):
                copy.start()

    for plane in range(2):
        for copy in writes(plane, CHUNKS - 1):
            copy.wait()


def solution(mesh):
    intervals, rows = mesh.shape["interval"], mesh.shape["rows"]

    def body(filtered, potential):
        x = filtered[0]
        n, cells = x.shape
        size = cells // 2
        width = size // CHUNKS
        pot = potential.reshape(1, cells)
        anywhere = pl.BlockSpec(memory_space=pl.ANY)
        vmem = pl.BlockSpec(memory_space=pltpu.VMEM)
        whole = jax.ShapeDtypeStruct((n, cells), F32)
        plane = jax.ShapeDtypeStruct((n, size), F32)
        dma = pltpu.SemaphoreType.DMA

        def kernel(*refs):
            exchange_kernel(intervals, rows, *refs)

        prev, low, high, plow, phigh, w, ritz = pl.pallas_call(
            kernel,
            out_shape=(
                whole, plane, plane, plane, plane,
                jax.ShapeDtypeStruct((2 * n, 4 * n), F32),
                jax.ShapeDtypeStruct((n, n), F32),
            ),
            in_specs=[anywhere, vmem],
            out_specs=(anywhere,) * 5 + (vmem, vmem),
            scratch_shapes=[
                pltpu.VMEM((n, cells), F32),
                pltpu.VMEM((n, cells), F32),
                pltpu.VMEM((n, size), F32),
                pltpu.VMEM((n, size), F32),
                *[pltpu.VMEM((n, width), F32) for _ in range(4)],
                pltpu.VMEM((4 * n, 4 * n), F32),
                pltpu.VMEM((3, 4, 2 * n, 2 * n), F32),
                pltpu.VMEM((2 * n, 2 * n), F32),
                pltpu.VMEM((n, 2 * n), F32),
                pltpu.VMEM((3, 4, n, 2 * n), F32),
                pltpu.VMEM((n, 2 * n), F32),
                pltpu.VMEM((n, 2 * n), F32),
                pltpu.VMEM((n, n), F32),
                dma((2 * CHUNKS,)), dma((2 * CHUNKS,)),
                dma((CHUNKS,)), dma((CHUNKS,)), dma((CHUNKS,)), dma((CHUNKS,)),
                dma((4,)), dma((4,)),
                dma((CHUNKS,)), dma((CHUNKS,)),
                dma((CHUNKS,)), dma((CHUNKS,)), dma((CHUNKS,)), dma((CHUNKS,)),
                dma((2 * CHUNKS,)), dma((4, CHUNKS)),
                dma((3, 4)), dma((3, 4)),
                dma, dma,
                dma((3, 4)), dma((3, 4)),
                dma, dma,
            ],
            compiler_params=pltpu.CompilerParams(
                collective_id=0, has_side_effects=True, vmem_limit_bytes=48 * 2**20
            ),
            name="exchange",
        )(x, pot)
        basis, residual = pl.pallas_call(
            apply_kernel,
            out_shape=(whole, whole),
            in_specs=[anywhere] * 6 + [vmem, vmem],
            out_specs=(anywhere, anywhere),
            scratch_shapes=[
                pltpu.VMEM((n, cells), F32),
                pltpu.VMEM((n, cells), F32),
                *[pltpu.VMEM((n, size), F32) for _ in range(4)],
                pltpu.VMEM((2, 2 * n, width), F32),
                dma((8, CHUNKS)), dma((2, 2)),
            ],
            compiler_params=pltpu.CompilerParams(vmem_limit_bytes=48 * 2**20),
            name="apply",
        )(x, prev, low, high, plow, phigh, pot, w)
        return basis[None], ritz[None], residual[None]

    return jax.shard_map(
        body,
        mesh=mesh,
        in_specs=(P("interval", None, "rows"), P("rows", None, None)),
        out_specs=(
            P("interval", None, "rows"),
            P("interval", None, None),
            P("interval", None, "rows"),
        ),
        check_vma=False,
    )
```

```python
import functools

import jax
import jax.numpy as jnp
from jax import lax
from jax.experimental import pallas as pl
from jax.experimental.pallas import tpu as pltpu
from jax.sharding import PartitionSpec as P

MESH = pl.DeviceIdType.MESH
F32 = jnp.float32
BF16 = jnp.bfloat16

LANES = 128
VMEM_EXCHANGE, VMEM_APPLY = 16 * 2**20, 8 * 2**20
LAYER = 16
CHUNKS = 8
RELAYS_UP = {0: 3, 1: 7, 2: 10, 5: 14, 6: 13, 7: 11}
RELAYS_DOWN = {0: 12, 1: 8, 2: 5, 5: 1, 6: 2, 7: 10}
LANDING = 4
FIRST_CROSS, THEN_CROSS = (6, 5), (4, 2, 0, 1, 3, 7)
ACROSS, BESIDE = (2, 5, 7), (0, 1, 3, 4, 6)
FIRST_ONWARD, NEXT_ONWARD = 2, 4
INVERT_AT = 5


def split(v):
    hi = v.astype(BF16)
    return hi, (v - hi.astype(F32)).astype(BF16)


def exact_dot(a, b, dims):
    return lax.dot_general(
        a, b, (dims, ((), ())), precision=lax.Precision.HIGHEST, preferred_element_type=F32
    )


def stencil(u, low, high, pot, plane, j, size, width):
    base = plane * size
    start = pl.multiple_of(base + j * width, LANES)
    c = u[:, pl.ds(start, width)]
    first = pl.multiple_of(jnp.maximum(start - LANES, base), LANES)
    last = pl.multiple_of(jnp.minimum(start + width, base + size - LANES), LANES)
    before = jnp.where(j > 0, u[:, pl.ds(first, LANES)], 0.0)
    after = jnp.where(j < size // width - 1, u[:, pl.ds(last, LANES)], 0.0)
    tiles = width // LANES
    part = [c[:, t * LANES : (t + 1) * LANES] for t in range(tiles)]
    around = [before, *part, after]
    lane = lax.broadcasted_iota(jnp.int32, part[0].shape, 1)
    other = u[:, pl.ds(pl.multiple_of((1 - plane) * size + j * width, LANES), width)]
    halo = (high if plane else low)[:, pl.ds(pl.multiple_of(j * width, LANES), width)]
    weight = 6.0 + pot[:, pl.ds(start, width)]
    out = []
    for t in range(tiles):
        cut = slice(t * LANES, (t + 1) * LANES)
        left = jnp.where(lane == 0, 0.0, pltpu.roll(part[t], 1, 1))
        right = jnp.where(lane == LANES - 1, 0.0, pltpu.roll(part[t], LANES - 1, 1))
        beside = (other[:, cut] + halo[:, cut]) + (around[t] + around[t + 2]) + (left + right)
        out.append(weight[:, cut] * part[t] - beside)
    return jnp.concatenate(out, axis=1)


def inverse_factor(square):
    n = square.shape[0]
    row = lax.broadcasted_iota(jnp.int32, (n, LANES), 0)
    lane = lax.broadcasted_iota(jnp.int32, (n, LANES), 1)
    t = jnp.where(lane < n, square, jnp.where(lane == row + n, 1.0, 0.0))
    for k in range(0, n, 2):
        top, under = t[k : k + 1, :], t[k + 1 : k + 2, :]
        one = 1.0 / t[k : k + 1, k : k + 1]
        ratio = t[k + 1 : k + 2, k : k + 1] * one
        first = jnp.broadcast_to(t[:, k : k + 1], (n, LANES))
        second = jnp.broadcast_to(t[:, k + 1 : k + 2], (n, LANES)) - first * ratio
        under = under - top * ratio
        two = 1.0 / (t[k + 1 : k + 2, k + 1 : k + 2] - t[k : k + 1, k + 1 : k + 2] * ratio)
        t = t - jnp.where(row > k, first, 0.0) * (top * one)
        t = t - jnp.where(row > k + 1, second, 0.0) * (under * two)
    diagonal = jnp.sum(jnp.where(lane == row, t, 0.0), axis=1, keepdims=True)
    t = t * (1.0 / jnp.sqrt(diagonal))
    return pltpu.roll(t, LANES - n, 1)[:, :n]


def coefficients(total, inv_p, prior, wait_prior, w_out, r_out):
    n = total.shape[0] // 2
    swapped = pltpu.roll(total, n, 1)
    gram, k_own = total[:n, :n], swapped[:n, :n]
    g_pi, k_pi = total[n:, :n], swapped[n:, :n]
    et = exact_dot(inv_p, g_pi, ((1,), (0,)))
    schur = gram - exact_dot(et, et, ((0,), (0,)))
    toward = exact_dot(et, inv_p, ((0,), (0,)))
    wide = jnp.concatenate([schur, jnp.zeros_like(schur)], axis=1)
    a = inverse_factor(wide)
    b = -exact_dot(a, toward, ((1,), (0,)))
    mixed = exact_dot(b, k_pi, ((1,), (0,)))
    ritz = exact_dot(exact_dot(a, k_own, ((1,), (0,))), a, ((1,), (1,)))
    ritz = ritz + exact_dot(mixed, a, ((1,), (1,))) + exact_dot(a, mixed, ((1,), (1,)))
    wait_prior()
    k_prior = pltpu.roll(prior[...], n, 1)[:, :n]
    ritz = ritz + exact_dot(exact_dot(b, k_prior, ((1,), (0,))), b, ((1,), (1,)))
    r_out[...] = ritz
    ra = exact_dot(ritz, a, ((0,), (0,)))
    rb = exact_dot(ritz, b, ((0,), (0,)))
    zero = jnp.zeros_like(a)
    w_out[:n, :] = jnp.concatenate([a, b, zero, zero], axis=1)
    w_out[n:, :] = jnp.concatenate([-ra, -rb, a, b], axis=1)


def exchange_kernel(
    intervals, rows,
    x, pot,
    prev, z_hi, z_lo, plow_o, phigh_o, w_o, r_o,
    low, high, up_a, up_b, down_a, down_b, acc, sums, total, prior, early_sums, early_total, early_prior, inv_p,
    x_send, x_recv, up_send, down_send, low_recv, high_recv,
    relay_send, relay_recv, pass_up_send, pass_down_send, plow_send, phigh_send, plow_recv, phigh_recv,
    sum_send, sum_recv, prior_send, prior_recv,
    early_send, early_recv, early_prior_send, early_prior_recv,
):
    i, r = lax.axis_index("interval"), lax.axis_index("rows")
    layers = rows // LAYER
    layer, q = r // LAYER, r % LAYER
    qx, qy = q // 4, q % 4
    size = low.shape[1]
    width = size // CHUNKS

    def at(c):
        return pl.ds(pl.multiple_of(c * width, LANES), width)

    def remote(src, dst, send, recv, to_i, to_r):
        return pltpu.make_async_remote_copy(
            src_ref=src, dst_ref=dst, send_sem=send, recv_sem=recv,
            device_id=(to_i, to_r), device_id_type=MESH,
        )

    barrier = pltpu.get_barrier_semaphore()

    def greet(to_i, to_r):
        pl.semaphore_signal(barrier, inc=1, device_id=(to_i, to_r), device_id_type=MESH)

    for d in range(1, layers):
        greet(i, lax.rem(layer + d, layers) * LAYER + q)
    for d in range(1, LAYER):
        greet(i, layer * LAYER + lax.rem(q + d, LAYER))
    has_prev, has_next = i > 0, i < intervals - 1
    has_low, has_high = r > 0, r < rows - 1
    for there, to_i, to_r in (
        (has_prev, i - 1, r), (has_next, i + 1, r), (has_low, i, r - 1), (has_high, i, r + 1)
    ):
        pl.when(there)(lambda to_i=to_i, to_r=to_r: greet(to_i, to_r))
    neighbours = (
        has_prev.astype(jnp.int32) + has_next.astype(jnp.int32)
        + has_low.astype(jnp.int32) + has_high.astype(jnp.int32)
    )
    n = prior.shape[0]
    early_acc = acc.at[pl.ds(0, 2 * n), pl.ds(0, 2 * n)]
    early_acc[...] = jnp.zeros((2 * n, 2 * n), F32)

    @pl.loop(0, 2 * CHUNKS)
    def _(c):
        both = jnp.concatenate(split(x[:, at(c)]), axis=0)
        early_acc[...] += lax.dot_general(
            both, both, (((1,), (1,)), ((), ())), preferred_element_type=F32
        )

    halves = early_acc[pl.ds(0, n), :] + pltpu.roll(early_acc[pl.ds(n, n), :], n, 1)
    own_gram = halves + pltpu.roll(halves, n, 1)
    pl.semaphore_wait(barrier, layers - 1 + LAYER - 1 + neighbours)

    places = (
        (qy, lambda o: r - qy + o), (qx, lambda o: r - qx * 4 + o * 4), (layer, lambda o: o * LAYER + q)
    )

    def sum_copy(buffer, send, recv, stage, slot, d, to_r):
        return remote(
            buffer.at[stage, slot], buffer.at[stage, slot], send.at[stage, d], recv.at[stage, slot], i, to_r)

    def sum_start(buffer, send, recv, stage, value):
        mine, place = places[stage]
        buffer[stage, mine] = value
        for d in range(1, 4):
            sum_copy(buffer, send, recv, stage, mine, d, place(lax.rem(mine + d, 4))).start()

    def sum_end(buffer, send, recv, stage):
        mine, _ = places[stage]
        for d in range(1, 4):
            sum_copy(buffer, send, recv, stage, lax.rem(mine + d, 4), d, r).wait_recv()
        return (buffer[stage, 0] + buffer[stage, 1]) + (buffer[stage, 2] + buffer[stage, 3])

    early = (early_sums, early_send, early_recv)
    late = (sums, sum_send, sum_recv)

    def summed(stage, value):
        sum_start(*late, stage, value)
        return sum_end(*late, stage)

    sum_start(*early, 0, own_gram)

    last_of_layer, first_of_layer = q == LAYER - 1, q == 0
    cross_up = jnp.logical_and(last_of_layer, has_high)
    cross_down = jnp.logical_and(first_of_layer, has_low)
    plain_up = jnp.logical_not(last_of_layer)
    plain_down = jnp.logical_not(first_of_layer)
    spare = relay_send.at[0]

    def up_plain(c):
        return remote(x.at[:, at(CHUNKS + c)], low.at[:, at(c)], up_send.at[c], low_recv.at[c], i, r + 1)

    def down_plain(c):
        return remote(x.at[:, at(c)], high.at[:, at(c)], down_send.at[c], high_recv.at[c], i, r - 1)

    base = layer * LAYER

    def up_cross(c):
        if c not in RELAYS_UP and c != LANDING:
            return up_plain(c)
        return remote(
            x.at[:, at(CHUNKS + c)], up_a, up_send.at[c], relay_recv.at[0], i, base + RELAYS_UP.get(c, 0))

    def down_cross(c):
        if c not in RELAYS_DOWN and c != LANDING:
            return down_plain(c)
        return remote(
            x.at[:, at(c)], down_a, down_send.at[c], relay_recv.at[2],
            i, base + RELAYS_DOWN.get(c, LAYER - 1))

    def onward(c):
        return remote(x.at[:, at(c)], prev.at[:, at(c)], x_send.at[c], x_recv.at[c], i + 1, r)

    def start_chunks(there, copies, chunks):
        @pl.when(there)
        def _():
            for c in chunks:
                for copy in copies:
                    copy(c).start()

    def onward_low(c):
        return onward(c)

    def onward_high(c):
        return onward(CHUNKS + c)

    def start_onward(first, last):
        start_chunks(has_next, (onward_low, onward_high), range(first, last))

    all_of = lambda *terms: functools.reduce(jnp.logical_and, terms)
    start_onward(0, FIRST_ONWARD)
    start_chunks(cross_up, (up_cross,), FIRST_CROSS)
    start_chunks(cross_down, (down_cross,), FIRST_CROSS)
    start_chunks(qy < 3, (up_plain,), range(CHUNKS))
    start_chunks(qy > 0, (down_plain,), range(CHUNKS))
    own_gram = sum_end(*early, 0)
    sum_start(*early, 1, own_gram)
    start_chunks(cross_up, (up_cross,), THEN_CROSS)
    start_chunks(cross_down, (down_cross,), THEN_CROSS)
    start_chunks(all_of(qy == 3, plain_up), (up_plain,), range(CHUNKS))
    start_chunks(all_of(qy == 0, plain_down), (down_plain,), range(CHUNKS))
    own_gram = sum_end(*early, 1)
    sum_start(*early, 2, own_gram)
    start_onward(FIRST_ONWARD, NEXT_ONWARD)

    acc[...] = jnp.zeros_like(acc)

    @pl.when(jnp.logical_not(has_prev))
    def _():
        prev[...] = jnp.zeros_like(prev)

    @pl.when(jnp.logical_not(has_low))
    def _():
        low[...] = jnp.zeros_like(low)

    @pl.when(jnp.logical_not(has_high))
    def _():
        high[...] = jnp.zeros_like(high)

    def role(table):
        chunk, first = jnp.int32(0), jnp.bool_(False)
        for c, of in table.items():
            chunk = chunk + jnp.where(q == of, c, 0)
            first = jnp.logical_or(first, q == of)
        return chunk, first

    up_chunk, up_relay = role(RELAYS_UP)
    down_chunk, down_relay = role(RELAYS_DOWN)
    above, below = layer < layers - 1, layer > 0
    first_hops = (
        (jnp.logical_and(up_relay, above), 0, up_a, remote(
            up_a, up_b, relay_send.at[0], relay_recv.at[1], i, r + LAYER)),
        (jnp.logical_and(down_relay, below), 2, down_a, remote(
            down_a, down_b, relay_send.at[2], relay_recv.at[3], i, r - LAYER)),
        (jnp.logical_and(first_of_layer, above), 0, up_a, remote(
            up_a, low.at[:, at(LANDING)], relay_send.at[0], low_recv.at[LANDING], i, r + LAYER)),
        (jnp.logical_and(last_of_layer, below), 2, down_a, remote(
            down_a, high.at[:, at(LANDING)], relay_send.at[2], high_recv.at[LANDING], i, r - LAYER)),
    )
    second_hops = (
        (jnp.logical_and(up_relay, below), 1, up_b, remote(
            up_b, low.at[:, at(up_chunk)], relay_send.at[1], low_recv.at[up_chunk], i, base)),
        (jnp.logical_and(down_relay, above), 3, down_b, remote(
            down_b, high.at[:, at(down_chunk)], relay_send.at[3], high_recv.at[down_chunk],
            i, base + LAYER - 1)),
    )

    def relay(hops):
        for there, slot, buffer, copy in hops:
            @pl.when(there)
            def _(slot=slot, buffer=buffer, copy=copy):
                remote(buffer, buffer, spare, relay_recv.at[slot], i, r).wait_recv()
                copy.start()

    relay(first_hops)
    start_onward(NEXT_ONWARD, CHUNKS)
    relay(second_hops)
    early_total[...] = sum_end(*early, 2)
    early_hand = remote(early_total, early_prior, early_prior_send, early_prior_recv, i + 1, r)
    pl.when(has_next)(lambda: early_hand.start())

    @pl.when(jnp.logical_not(has_prev))
    def _():
        row = lax.broadcasted_iota(jnp.int32, early_prior.shape, 0)
        lane = lax.broadcasted_iota(jnp.int32, early_prior.shape, 1)
        early_prior[...] = jnp.where(row == lane, 1.0, 0.0)
        prior[...] = jnp.zeros_like(prior)


    gives = lax.rem(i, 2) == 0
    across = jnp.logical_and(has_next, jnp.logical_not(gives))

    def give_low(c):
        return remote(low.at[:, at(c)], plow_o.at[:, at(c)], plow_send.at[c], plow_recv.at[c], i + 1, r)

    def give_high(c):
        return remote(high.at[:, at(c)], phigh_o.at[:, at(c)], phigh_send.at[c], phigh_recv.at[c], i + 1, r)

    lone = jnp.logical_and(has_prev, gives)

    def invert():
        pl.when(has_prev)(lambda: early_hand.wait_recv())
        inv_p[...] = inverse_factor(early_prior[...])

    crossed = jnp.logical_or(cross_up, cross_down).astype(jnp.int32)

    @pl.loop(0, CHUNKS)
    def _(step):
        c = lax.rem(step + crossed, CHUNKS)
        pl.when(jnp.logical_and(step == INVERT_AT, jnp.logical_not(lone)))(invert)

        @pl.when(has_prev)
        def _():
            onward(c).wait_recv()
            onward(CHUNKS + c).wait_recv()

        @pl.when(has_low)
        def _():
            up_plain(c).wait_recv()

        @pl.when(has_high)
        def _():
            down_plain(c).wait_recv()

        @pl.when(gives)
        def _():
            give_low(c).start()
            give_high(c).start()

        for plane in range(2):
            mine = x[:, at(plane * CHUNKS + c)]
            image = stencil(x, low, high, pot, plane, c, size, width)
            theirs = prev[:, at(plane * CHUNKS + c)]
            mine_hi, mine_lo = split(mine)
            image_hi, image_lo = split(image)
            theirs_hi, theirs_lo = split(theirs)
            where = at(plane * CHUNKS + c)
            z_hi[:, where] = jnp.concatenate([mine_hi, theirs_hi, image_hi], axis=0)
            z_lo[:, where] = jnp.concatenate([mine_lo, theirs_lo, image_lo], axis=0)
            left = jnp.concatenate([mine_hi, theirs_hi, mine_lo, theirs_lo], axis=0)
            right = jnp.concatenate([mine_hi, image_hi, mine_lo, image_lo], axis=0)
            acc[...] += lax.dot_general(
                left, right, (((1,), (1,)), ((), ())), preferred_element_type=F32
            )

    half = acc.shape[0] // 2
    partial = acc[:half, :half] + acc[half:, half:] + (acc[:half, half:] + acc[half:, :half])

    def pass_up(c):
        return remote(
            prev.at[:, at(CHUNKS + c)], plow_o.at[:, at(c)], pass_up_send.at[c], plow_recv.at[c], i, r + 1)

    def pass_down(c):
        return remote(
            prev.at[:, at(c)], phigh_o.at[:, at(c)], pass_down_send.at[c], phigh_recv.at[c], i, r - 1)

    def none_low(c):
        return pltpu.make_async_copy(prev.at[:, at(c)], plow_o.at[:, at(c)], plow_recv.at[c])

    def none_high(c):
        return pltpu.make_async_copy(prev.at[:, at(c)], phigh_o.at[:, at(c)], phigh_recv.at[c])

    def own_low(c):
        return pltpu.make_async_copy(low.at[:, at(c)], plow_o.at[:, at(c)], plow_recv.at[c])

    def own_high(c):
        return pltpu.make_async_copy(high.at[:, at(c)], phigh_o.at[:, at(c)], phigh_recv.at[c])

    start_chunks(jnp.logical_not(has_prev), (none_low, none_high), range(CHUNKS))
    start_chunks(all_of(lone, jnp.logical_not(has_low)), (own_low,), BESIDE)
    start_chunks(all_of(lone, jnp.logical_not(has_high)), (own_high,), BESIDE)
    passes = (
        (all_of(lone, qy < 3), pass_up, BESIDE),
        (all_of(lone, q == LAYER - 2, above), pass_up, ACROSS),
        (all_of(lone, qy > 0), pass_down, BESIDE),
        (all_of(lone, q == 1, below), pass_down, ACROSS),
        (all_of(lone, qy == 3, plain_up), pass_up, BESIDE),
        (all_of(lone, qy == 0, plain_down), pass_down, BESIDE),
    )
    only_high, only_low = jnp.logical_and(across, cross_up), jnp.logical_and(across, cross_down)
    not_up = jnp.logical_and(across, jnp.logical_not(cross_up))
    not_down = jnp.logical_and(across, jnp.logical_not(cross_down))

    sum_start(*late, 0, partial)
    for there, copy, chunks in passes[:4]:
        start_chunks(there, (copy,), chunks)
    start_chunks(only_low, (give_low,), BESIDE[:2])
    start_chunks(only_high, (give_high,), BESIDE[:2])
    pl.when(lone)(invert)
    partial = sum_end(*late, 0)
    partial = summed(1, partial)
    for there, copy, chunks in passes[4:]:
        start_chunks(there, (copy,), chunks)
    sum_start(*late, 2, partial)
    start_chunks(not_up, (give_low,), ACROSS[:1])
    start_chunks(not_down, (give_high,), ACROSS[:1])
    total[...] = sum_end(*late, 2)
    hand = remote(total.at[pl.ds(0, n)], prior, prior_send, prior_recv, i + 1, r)
    pl.when(has_next)(lambda: hand.start())
    start_chunks(not_up, (give_low,), ACROSS[1:])
    start_chunks(not_down, (give_high,), ACROSS[1:])
    start_chunks(only_low, (give_low,), BESIDE[2:])
    start_chunks(only_high, (give_high,), BESIDE[2:])
    wait_prior = lambda: pl.when(has_prev)(lambda: hand.wait_recv())
    coefficients(total[...], inv_p[...], prior, wait_prior, w_o, r_o)

    for c in range(CHUNKS):
        give_low(c).wait_recv()
        give_high(c).wait_recv()

    def end_chunks(there, copies, chunks):
        @pl.when(there)
        def _():
            for c in chunks:
                for copy in copies:
                    copy(c).wait_send()

    end_chunks(has_high, (up_plain,), range(CHUNKS))
    end_chunks(has_low, (down_plain,), range(CHUNKS))
    pl.when(has_next)(lambda: hand.wait_send())
    pl.when(has_next)(lambda: early_hand.wait_send())
    end_chunks(has_next, (onward,), range(2 * CHUNKS))
    end_chunks(gives, (give_low, give_high), range(CHUNKS))
    end_chunks(not_up, (give_low,), ACROSS)
    end_chunks(not_down, (give_high,), ACROSS)
    end_chunks(only_low, (give_low,), BESIDE)
    end_chunks(only_high, (give_high,), BESIDE)
    for there, copy, chunks in passes:
        end_chunks(there, (copy,), chunks)
    for there, _, _, copy in first_hops + second_hops:
        pl.when(there)(lambda copy=copy: copy.wait_send())

    for stage in range(3):
        for d in range(1, 4):
            sum_copy(*early, stage, 0, d, r).wait_send()
            sum_copy(*late, stage, 0, d, r).wait_send()


def apply_kernel(
    prev, z_hi, z_lo, plow, phigh, pot, w, r, basis_o, ritz_o, residual_o, out, out_sem, ritz_sem
):
    size = plow.shape[1]
    width = size // CHUNKS
    n = prev.shape[0]
    ritz = pltpu.make_async_copy(r, ritz_o, ritz_sem)
    ritz.start()

    def at(c):
        return pl.ds(pl.multiple_of(c * width, LANES), width)

    def writes(plane, c):
        where = at(plane * CHUNKS + c)
        return [
            pltpu.make_async_copy(out.at[plane, pl.ds(e * n, n)], dst.at[:, where], out_sem.at[plane, e])
            for e, dst in enumerate((basis_o, residual_o))
        ]

    w_hi, w_lo = split(w[...])
    both = jnp.concatenate([w_hi, w_lo], axis=0)

    @pl.loop(0, CHUNKS)
    def _(c):
        for plane in range(2):
            where = at(plane * CHUNKS + c)
            image_hi, image_lo = split(stencil(prev, plow, phigh, pot, plane, c, size, width))
            wide = jnp.dot(
                both, jnp.concatenate([z_hi[:, where], image_hi], axis=0), preferred_element_type=F32
            )
            narrow = jnp.dot(
                w_hi, jnp.concatenate([z_lo[:, where], image_lo], axis=0), preferred_element_type=F32
            )
            value = (wide[: 2 * n] + wide[2 * n :]) + narrow

            @pl.when(c > 0)
            def _():
                for copy in writes(plane, c - 1):
                    copy.wait()

            out[plane] = value
            for copy in writes(plane, c):
                copy.start()

    for plane in range(2):
        for copy in writes(plane, CHUNKS - 1):
            copy.wait()
    ritz.wait()


def solution(mesh):
    intervals, rows = mesh.shape["interval"], mesh.shape["rows"]

    def body(filtered, potential):
        x = filtered[0]
        n, cells = x.shape
        size = cells // 2
        width = size // CHUNKS
        pot = potential.reshape(1, cells)
        hbm = pl.BlockSpec(memory_space=pltpu.HBM)
        vmem = pl.BlockSpec(memory_space=pltpu.VMEM)
        whole = jax.ShapeDtypeStruct((n, cells), F32)
        plane = jax.ShapeDtypeStruct((n, size), F32)
        dma = pltpu.SemaphoreType.DMA

        def kernel(*refs):
            exchange_kernel(intervals, rows, *refs)

        stack = jax.ShapeDtypeStruct((3 * n, cells), BF16)
        prev, z_hi, z_lo, plow, phigh, w, r = pl.pallas_call(
            kernel,
            out_shape=(
                whole, stack, stack, plane, plane,
                jax.ShapeDtypeStruct((2 * n, 4 * n), F32),
                jax.ShapeDtypeStruct((n, n), F32),
            ),
            in_specs=[vmem, vmem],
            out_specs=(vmem,) * 7,
            scratch_shapes=[
                pltpu.VMEM((n, size), F32),
                pltpu.VMEM((n, size), F32),
                *[pltpu.VMEM((n, width), F32) for _ in range(4)],
                pltpu.VMEM((4 * n, 4 * n), F32),
                pltpu.VMEM((3, 4, 2 * n, 2 * n), F32),
                pltpu.VMEM((2 * n, 2 * n), F32),
                pltpu.VMEM((n, 2 * n), F32),
                pltpu.VMEM((3, 4, n, 2 * n), F32),
                pltpu.VMEM((n, 2 * n), F32),
                pltpu.VMEM((n, 2 * n), F32),
                pltpu.VMEM((n, n), F32),
                dma((2 * CHUNKS,)), dma((2 * CHUNKS,)),
                dma((CHUNKS,)), dma((CHUNKS,)), dma((CHUNKS,)), dma((CHUNKS,)),
                dma((4,)), dma((4,)),
                dma((CHUNKS,)), dma((CHUNKS,)),
                dma((CHUNKS,)), dma((CHUNKS,)), dma((CHUNKS,)), dma((CHUNKS,)),
                dma((3, 4)), dma((3, 4)),
                dma, dma,
                dma((3, 4)), dma((3, 4)),
                dma, dma,
            ],
            compiler_params=pltpu.CompilerParams(
                collective_id=0, has_side_effects=True, vmem_limit_bytes=VMEM_EXCHANGE
            ),
            name="exchange",
        )(x, pot)
        basis, ritz, residual = pl.pallas_call(
            apply_kernel,
            out_shape=(whole, jax.ShapeDtypeStruct((n, n), F32), whole),
            in_specs=[vmem] * 8,
            out_specs=(hbm,) * 3,
            scratch_shapes=[pltpu.VMEM((2, 2 * n, width), F32), dma((2, 2)), dma],
            compiler_params=pltpu.CompilerParams(vmem_limit_bytes=VMEM_APPLY),
            name="apply",
        )(prev, z_hi, z_lo, plow, phigh, pot, w, r)
        return basis[None], ritz[None], residual[None]

    return jax.shard_map(
        body,
        mesh=mesh,
        in_specs=(P("interval", None, "rows"), P("rows", None, None)),
        out_specs=(
            P("interval", None, "rows"),
            P("interval", None, None),
            P("interval", None, "rows"),
        ),
        check_vma=False,
    )
```

```python
import functools

import jax
import jax.numpy as jnp
from jax import lax
from jax.experimental import pallas as pl
from jax.experimental.pallas import tpu as pltpu
from jax.sharding import PartitionSpec as P

MESH = pl.DeviceIdType.MESH
F32 = jnp.float32
BF16 = jnp.bfloat16

LANES = 128
VMEM_EXCHANGE, VMEM_APPLY = 16 * 2**20, 8 * 2**20
LAYER = 16
CHUNKS = 8
RELAYS_UP = {0: 3, 1: 7, 2: 10, 5: 14, 6: 13, 7: 11}
RELAYS_DOWN = {0: 12, 1: 8, 2: 5, 5: 1, 6: 2, 7: 10}
LANDING = 4
FIRST_CROSS, THEN_CROSS = (6, 5), (4, 2, 0, 1, 3, 7)
ACROSS, BESIDE = (2, 5, 7), (0, 1, 3, 4, 6)
FIRST_ONWARD, NEXT_ONWARD = 2, 4
INVERT_AT = 5


def split(v):
    hi = v.astype(BF16)
    return hi, (v - hi.astype(F32)).astype(BF16)


def exact_dot(a, b, dims):
    return lax.dot_general(
        a, b, (dims, ((), ())), precision=lax.Precision.HIGHEST, preferred_element_type=F32
    )


def stencil(u, low, high, pot, plane, j, size, width):
    base = plane * size
    start = pl.multiple_of(base + j * width, LANES)
    c = u[:, pl.ds(start, width)]
    first = pl.multiple_of(jnp.maximum(start - LANES, base), LANES)
    last = pl.multiple_of(jnp.minimum(start + width, base + size - LANES), LANES)
    before = jnp.where(j > 0, u[:, pl.ds(first, LANES)], 0.0)
    after = jnp.where(j < size // width - 1, u[:, pl.ds(last, LANES)], 0.0)
    tiles = width // LANES
    part = [c[:, t * LANES : (t + 1) * LANES] for t in range(tiles)]
    around = [before, *part, after]
    lane = lax.broadcasted_iota(jnp.int32, part[0].shape, 1)
    other = u[:, pl.ds(pl.multiple_of((1 - plane) * size + j * width, LANES), width)]
    halo = (high if plane else low)[:, pl.ds(pl.multiple_of(j * width, LANES), width)]
    weight = 6.0 + pot[:, pl.ds(start, width)]
    out = []
    for t in range(tiles):
        cut = slice(t * LANES, (t + 1) * LANES)
        left = jnp.where(lane == 0, 0.0, pltpu.roll(part[t], 1, 1))
        right = jnp.where(lane == LANES - 1, 0.0, pltpu.roll(part[t], LANES - 1, 1))
        beside = (other[:, cut] + halo[:, cut]) + (around[t] + around[t + 2]) + (left + right)
        out.append(weight[:, cut] * part[t] - beside)
    return jnp.concatenate(out, axis=1)


def inverse_factor(square):
    n = square.shape[0]
    row = lax.broadcasted_iota(jnp.int32, (n, LANES), 0)
    lane = lax.broadcasted_iota(jnp.int32, (n, LANES), 1)
    t = jnp.where(lane < n, square, jnp.where(lane == row + n, 1.0, 0.0))
    rows = [t[b : b + 8] for b in range(0, n, 8)]
    shape = (8, LANES)
    place = lax.broadcasted_iota(jnp.int32, shape, 0)
    for k in range(0, n, 2):
        at, own = k % 8, rows[k // 8]
        top, under = own[at : at + 1, :], own[at + 1 : at + 2, :]
        one = 1.0 / own[at : at + 1, k : k + 1]
        ratio = own[at + 1 : at + 2, k : k + 1] * one
        under = under - top * ratio
        two = 1.0 / (own[at + 1 : at + 2, k + 1 : k + 2] - own[at : at + 1, k + 1 : k + 2] * ratio)
        scaled, scaled_under = top * one, under * two
        for b in range(k // 8, n // 8):
            first = jnp.broadcast_to(rows[b][:, k : k + 1], shape)
            second = jnp.broadcast_to(rows[b][:, k + 1 : k + 2], shape) - first * ratio
            if b == k // 8:
                first = jnp.where(place > at, first, 0.0)
                second = jnp.where(place > at + 1, second, 0.0)
            rows[b] = rows[b] - first * scaled - second * scaled_under
    t = jnp.concatenate(rows, axis=0)
    diagonal = jnp.sum(jnp.where(lane == row, t, 0.0), axis=1, keepdims=True)
    t = t * (1.0 / jnp.sqrt(diagonal))
    return pltpu.roll(t, LANES - n, 1)[:, :n]


def pack(upper, lower):
    lane = lax.broadcasted_iota(jnp.int32, upper.shape, 1)
    return jnp.where(lane < LANES // 2, upper, lower)


def unpack(packed):
    return jnp.concatenate([packed, pltpu.roll(packed, LANES // 2, 1)], axis=0)


def coefficients(own, total, inv_p, prior, wait_prior, w_out, r_out):
    n = total.shape[0] - own.shape[0]
    gram = unpack(own)[:, :n]
    g_pi, k_pi = total[:n, :n], pltpu.roll(total[:n], n, 1)[:, :n]
    k_own = unpack(total[n:])[:, :n]
    et = exact_dot(inv_p, g_pi, ((1,), (0,)))
    schur = gram - exact_dot(et, et, ((0,), (0,)))
    toward = exact_dot(et, inv_p, ((0,), (0,)))
    wide = jnp.concatenate([schur, jnp.zeros_like(schur)], axis=1)
    a = inverse_factor(wide)
    b = -exact_dot(a, toward, ((1,), (0,)))
    mixed = exact_dot(b, k_pi, ((1,), (0,)))
    ritz = exact_dot(exact_dot(a, k_own, ((1,), (0,))), a, ((1,), (1,)))
    ritz = ritz + exact_dot(mixed, a, ((1,), (1,))) + exact_dot(a, mixed, ((1,), (1,)))
    wait_prior()
    k_prior = unpack(prior[...])[:, :n]
    ritz = ritz + exact_dot(exact_dot(b, k_prior, ((1,), (0,))), b, ((1,), (1,)))
    r_out[...] = ritz
    ra = exact_dot(ritz, a, ((0,), (0,)))
    rb = exact_dot(ritz, b, ((0,), (0,)))
    zero = jnp.zeros_like(a)
    w_out[:n, :] = jnp.concatenate([a, b, zero, zero], axis=1)
    w_out[n:, :] = jnp.concatenate([-ra, -rb, a, b], axis=1)


def exchange_kernel(
    intervals, rows,
    x, pot,
    prev, z_hi, z_lo, plow_o, phigh_o, w_o, r_o,
    low, high, up_a, up_b, down_a, down_b, acc, sums, total, prior, early_sums, early_total, early_prior, inv_p,
    x_send, x_recv, up_send, down_send, low_recv, high_recv,
    relay_send, relay_recv, pass_up_send, pass_down_send, plow_send, phigh_send, plow_recv, phigh_recv,
    sum_send, sum_recv, prior_send, prior_recv,
    early_send, early_recv, early_prior_send, early_prior_recv,
):
    i, r = lax.axis_index("interval"), lax.axis_index("rows")
    layers = rows // LAYER
    layer, q = r // LAYER, r % LAYER
    qx, qy = q // 4, q % 4
    size = low.shape[1]
    width = size // CHUNKS

    def at(c):
        return pl.ds(pl.multiple_of(c * width, LANES), width)

    def remote(src, dst, send, recv, to_i, to_r):
        return pltpu.make_async_remote_copy(
            src_ref=src, dst_ref=dst, send_sem=send, recv_sem=recv,
            device_id=(to_i, to_r), device_id_type=MESH,
        )

    barrier = pltpu.get_barrier_semaphore()

    def greet(to_i, to_r):
        pl.semaphore_signal(barrier, inc=1, device_id=(to_i, to_r), device_id_type=MESH)

    for d in range(1, layers):
        greet(i, lax.rem(layer + d, layers) * LAYER + q)
    for d in range(1, LAYER):
        greet(i, layer * LAYER + lax.rem(q + d, LAYER))
    has_prev, has_next = i > 0, i < intervals - 1
    has_low, has_high = r > 0, r < rows - 1
    for there, to_i, to_r in (
        (has_prev, i - 1, r), (has_next, i + 1, r), (has_low, i, r - 1), (has_high, i, r + 1)
    ):
        pl.when(there)(lambda to_i=to_i, to_r=to_r: greet(to_i, to_r))
    neighbours = (
        has_prev.astype(jnp.int32) + has_next.astype(jnp.int32)
        + has_low.astype(jnp.int32) + has_high.astype(jnp.int32)
    )
    n = acc.shape[0] // 4
    early_acc = acc.at[pl.ds(0, 2 * n), pl.ds(0, 2 * n)]
    early_acc[...] = jnp.zeros((2 * n, 2 * n), F32)

    @pl.loop(0, 2 * CHUNKS)
    def _(c):
        both = jnp.concatenate(split(x[:, at(c)]), axis=0)
        early_acc[...] += lax.dot_general(
            both, both, (((1,), (1,)), ((), ())), preferred_element_type=F32
        )

    halves = early_acc[pl.ds(0, n), :] + pltpu.roll(early_acc[pl.ds(n, n), :], n, 1)
    own_gram = halves + pltpu.roll(halves, n, 1)
    own_gram = pack(own_gram[: n // 2], own_gram[n // 2 :])
    pl.semaphore_wait(barrier, layers - 1 + LAYER - 1 + neighbours)

    places = (
        (qy, lambda o: r - qy + o), (qx, lambda o: r - qx * 4 + o * 4), (layer, lambda o: o * LAYER + q)
    )

    def sum_copy(buffer, send, recv, stage, slot, d, to_r):
        return remote(
            buffer.at[stage, slot], buffer.at[stage, slot], send.at[stage, d], recv.at[stage, slot], i, to_r)

    def sum_start(buffer, send, recv, stage, value):
        mine, place = places[stage]
        buffer[stage, mine] = value
        for d in range(1, 4):
            sum_copy(buffer, send, recv, stage, mine, d, place(lax.rem(mine + d, 4))).start()

    def sum_end(buffer, send, recv, stage):
        mine, _ = places[stage]
        for d in range(1, 4):
            sum_copy(buffer, send, recv, stage, lax.rem(mine + d, 4), d, r).wait_recv()
        return (buffer[stage, 0] + buffer[stage, 1]) + (buffer[stage, 2] + buffer[stage, 3])

    early = (early_sums, early_send, early_recv)
    late = (sums, sum_send, sum_recv)

    def summed(stage, value):
        sum_start(*late, stage, value)
        return sum_end(*late, stage)

    sum_start(*early, 0, own_gram)

    last_of_layer, first_of_layer = q == LAYER - 1, q == 0
    cross_up = jnp.logical_and(last_of_layer, has_high)
    cross_down = jnp.logical_and(first_of_layer, has_low)
    plain_up = jnp.logical_not(last_of_layer)
    plain_down = jnp.logical_not(first_of_layer)
    spare = relay_send.at[0]

    def up_plain(c):
        return remote(x.at[:, at(CHUNKS + c)], low.at[:, at(c)], up_send.at[c], low_recv.at[c], i, r + 1)

    def down_plain(c):
        return remote(x.at[:, at(c)], high.at[:, at(c)], down_send.at[c], high_recv.at[c], i, r - 1)

    base = layer * LAYER

    def up_cross(c):
        if c not in RELAYS_UP and c != LANDING:
            return up_plain(c)
        return remote(
            x.at[:, at(CHUNKS + c)], up_a, up_send.at[c], relay_recv.at[0], i, base + RELAYS_UP.get(c, 0))

    def down_cross(c):
        if c not in RELAYS_DOWN and c != LANDING:
            return down_plain(c)
        return remote(
            x.at[:, at(c)], down_a, down_send.at[c], relay_recv.at[2],
            i, base + RELAYS_DOWN.get(c, LAYER - 1))

    def onward(c):
        return remote(x.at[:, at(c)], prev.at[:, at(c)], x_send.at[c], x_recv.at[c], i + 1, r)

    def start_chunks(there, copies, chunks):
        @pl.when(there)
        def _():
            for c in chunks:
                for copy in copies:
                    copy(c).start()

    def onward_low(c):
        return onward(c)

    def onward_high(c):
        return onward(CHUNKS + c)

    def start_onward(first, last):
        start_chunks(has_next, (onward_low, onward_high), range(first, last))

    all_of = lambda *terms: functools.reduce(jnp.logical_and, terms)
    start_onward(0, FIRST_ONWARD)
    start_chunks(cross_up, (up_cross,), FIRST_CROSS)
    start_chunks(cross_down, (down_cross,), FIRST_CROSS)
    start_chunks(qy < 3, (up_plain,), range(CHUNKS))
    start_chunks(qy > 0, (down_plain,), range(CHUNKS))
    own_gram = sum_end(*early, 0)
    sum_start(*early, 1, own_gram)
    start_chunks(cross_up, (up_cross,), THEN_CROSS)
    start_chunks(cross_down, (down_cross,), THEN_CROSS)
    start_chunks(all_of(qy == 3, plain_up), (up_plain,), range(CHUNKS))
    start_chunks(all_of(qy == 0, plain_down), (down_plain,), range(CHUNKS))
    own_gram = sum_end(*early, 1)
    sum_start(*early, 2, own_gram)
    start_onward(FIRST_ONWARD, NEXT_ONWARD)

    acc[...] = jnp.zeros_like(acc)

    @pl.when(jnp.logical_not(has_prev))
    def _():
        prev[...] = jnp.zeros_like(prev)

    @pl.when(jnp.logical_not(has_low))
    def _():
        low[...] = jnp.zeros_like(low)

    @pl.when(jnp.logical_not(has_high))
    def _():
        high[...] = jnp.zeros_like(high)

    def role(table):
        chunk, first = jnp.int32(0), jnp.bool_(False)
        for c, of in table.items():
            chunk = chunk + jnp.where(q == of, c, 0)
            first = jnp.logical_or(first, q == of)
        return chunk, first

    up_chunk, up_relay = role(RELAYS_UP)
    down_chunk, down_relay = role(RELAYS_DOWN)
    above, below = layer < layers - 1, layer > 0
    first_hops = (
        (jnp.logical_and(up_relay, above), 0, up_a, remote(
            up_a, up_b, relay_send.at[0], relay_recv.at[1], i, r + LAYER)),
        (jnp.logical_and(down_relay, below), 2, down_a, remote(
            down_a, down_b, relay_send.at[2], relay_recv.at[3], i, r - LAYER)),
        (jnp.logical_and(first_of_layer, above), 0, up_a, remote(
            up_a, low.at[:, at(LANDING)], relay_send.at[0], low_recv.at[LANDING], i, r + LAYER)),
        (jnp.logical_and(last_of_layer, below), 2, down_a, remote(
            down_a, high.at[:, at(LANDING)], relay_send.at[2], high_recv.at[LANDING], i, r - LAYER)),
    )
    second_hops = (
        (jnp.logical_and(up_relay, below), 1, up_b, remote(
            up_b, low.at[:, at(up_chunk)], relay_send.at[1], low_recv.at[up_chunk], i, base)),
        (jnp.logical_and(down_relay, above), 3, down_b, remote(
            down_b, high.at[:, at(down_chunk)], relay_send.at[3], high_recv.at[down_chunk],
            i, base + LAYER - 1)),
    )

    def relay(hops):
        for there, slot, buffer, copy in hops:
            @pl.when(there)
            def _(slot=slot, buffer=buffer, copy=copy):
                remote(buffer, buffer, spare, relay_recv.at[slot], i, r).wait_recv()
                copy.start()

    relay(first_hops)
    start_onward(NEXT_ONWARD, CHUNKS)
    relay(second_hops)
    early_total[...] = sum_end(*early, 2)
    early_hand = remote(early_total, early_prior, early_prior_send, early_prior_recv, i + 1, r)
    pl.when(has_next)(lambda: early_hand.start())

    @pl.when(jnp.logical_not(has_prev))
    def _():
        row = lax.broadcasted_iota(jnp.int32, early_prior.shape, 0)
        lane = lax.broadcasted_iota(jnp.int32, early_prior.shape, 1)
        early_prior[...] = jnp.where(lax.rem(lane, n) == row + n // 2 * (lane // n), 1.0, 0.0)
        prior[...] = jnp.zeros_like(prior)


    gives = lax.rem(i, 2) == 0
    across = jnp.logical_and(has_next, jnp.logical_not(gives))

    def give_low(c):
        return remote(low.at[:, at(c)], plow_o.at[:, at(c)], plow_send.at[c], plow_recv.at[c], i + 1, r)

    def give_high(c):
        return remote(high.at[:, at(c)], phigh_o.at[:, at(c)], phigh_send.at[c], phigh_recv.at[c], i + 1, r)

    lone = jnp.logical_and(has_prev, gives)

    def invert():
        pl.when(has_prev)(lambda: early_hand.wait_recv())
        inv_p[...] = inverse_factor(unpack(early_prior[...]))

    crossed = jnp.logical_or(cross_up, cross_down).astype(jnp.int32)

    @pl.loop(0, CHUNKS)
    def _(step):
        c = lax.rem(step + crossed, CHUNKS)
        pl.when(jnp.logical_and(step == INVERT_AT, jnp.logical_not(lone)))(invert)

        @pl.when(has_prev)
        def _():
            onward(c).wait_recv()
            onward(CHUNKS + c).wait_recv()

        @pl.when(has_low)
        def _():
            up_plain(c).wait_recv()

        @pl.when(has_high)
        def _():
            down_plain(c).wait_recv()

        @pl.when(gives)
        def _():
            give_low(c).start()
            give_high(c).start()

        for plane in range(2):
            mine = x[:, at(plane * CHUNKS + c)]
            image = stencil(x, low, high, pot, plane, c, size, width)
            theirs = prev[:, at(plane * CHUNKS + c)]
            mine_hi, mine_lo = split(mine)
            image_hi, image_lo = split(image)
            theirs_hi, theirs_lo = split(theirs)
            where = at(plane * CHUNKS + c)
            z_hi[:, where] = jnp.concatenate([mine_hi, theirs_hi, image_hi], axis=0)
            z_lo[:, where] = jnp.concatenate([mine_lo, theirs_lo, image_lo], axis=0)
            left = jnp.concatenate([mine_hi, theirs_hi, mine_lo, theirs_lo], axis=0)
            right = jnp.concatenate([mine_hi, image_hi, mine_lo, image_lo], axis=0)
            acc[...] += lax.dot_general(
                left, right, (((1,), (1,)), ((), ())), preferred_element_type=F32
            )

    half = acc.shape[0] // 2
    partial = acc[:half, :half] + acc[half:, half:] + (acc[:half, half:] + acc[half:, :half])
    square = pltpu.roll(partial[: n // 2], n, 1)
    partial = jnp.concatenate([partial[n:], pack(square, partial[n // 2 : n])], axis=0)

    def pass_up(c):
        return remote(
            prev.at[:, at(CHUNKS + c)], plow_o.at[:, at(c)], pass_up_send.at[c], plow_recv.at[c], i, r + 1)

    def pass_down(c):
        return remote(
            prev.at[:, at(c)], phigh_o.at[:, at(c)], pass_down_send.at[c], phigh_recv.at[c], i, r - 1)

    def none_low(c):
        return pltpu.make_async_copy(prev.at[:, at(c)], plow_o.at[:, at(c)], plow_recv.at[c])

    def none_high(c):
        return pltpu.make_async_copy(prev.at[:, at(c)], phigh_o.at[:, at(c)], phigh_recv.at[c])

    def own_low(c):
        return pltpu.make_async_copy(low.at[:, at(c)], plow_o.at[:, at(c)], plow_recv.at[c])

    def own_high(c):
        return pltpu.make_async_copy(high.at[:, at(c)], phigh_o.at[:, at(c)], phigh_recv.at[c])

    start_chunks(jnp.logical_not(has_prev), (none_low, none_high), range(CHUNKS))
    start_chunks(all_of(lone, jnp.logical_not(has_low)), (own_low,), BESIDE)
    start_chunks(all_of(lone, jnp.logical_not(has_high)), (own_high,), BESIDE)
    passes = (
        (all_of(lone, qy < 3), pass_up, BESIDE),
        (all_of(lone, q == LAYER - 2, above), pass_up, ACROSS),
        (all_of(lone, qy > 0), pass_down, BESIDE),
        (all_of(lone, q == 1, below), pass_down, ACROSS),
        (all_of(lone, qy == 3, plain_up), pass_up, BESIDE),
        (all_of(lone, qy == 0, plain_down), pass_down, BESIDE),
    )
    only_high, only_low = jnp.logical_and(across, cross_up), jnp.logical_and(across, cross_down)
    not_up = jnp.logical_and(across, jnp.logical_not(cross_up))
    not_down = jnp.logical_and(across, jnp.logical_not(cross_down))

    sum_start(*late, 0, partial)
    for there, copy, chunks in passes[:4]:
        start_chunks(there, (copy,), chunks)
    start_chunks(only_low, (give_low,), BESIDE[:2])
    start_chunks(only_high, (give_high,), BESIDE[:2])
    pl.when(lone)(invert)
    partial = sum_end(*late, 0)
    partial = summed(1, partial)
    for there, copy, chunks in passes[4:]:
        start_chunks(there, (copy,), chunks)
    sum_start(*late, 2, partial)
    start_chunks(not_up, (give_low,), ACROSS[:1])
    start_chunks(not_down, (give_high,), ACROSS[:1])
    total[...] = sum_end(*late, 2)
    hand = remote(total.at[pl.ds(n, n // 2)], prior, prior_send, prior_recv, i + 1, r)
    pl.when(has_next)(lambda: hand.start())
    start_chunks(not_up, (give_low,), ACROSS[1:])
    start_chunks(not_down, (give_high,), ACROSS[1:])
    start_chunks(only_low, (give_low,), BESIDE[2:])
    start_chunks(only_high, (give_high,), BESIDE[2:])
    wait_prior = lambda: pl.when(has_prev)(lambda: hand.wait_recv())
    coefficients(early_total[...], total[...], inv_p[...], prior, wait_prior, w_o, r_o)

    for c in range(CHUNKS):
        give_low(c).wait_recv()
        give_high(c).wait_recv()

    def end_chunks(there, copies, chunks):
        @pl.when(there)
        def _():
            for c in chunks:
                for copy in copies:
                    copy(c).wait_send()

    end_chunks(has_high, (up_plain,), range(CHUNKS))
    end_chunks(has_low, (down_plain,), range(CHUNKS))
    pl.when(has_next)(lambda: hand.wait_send())
    pl.when(has_next)(lambda: early_hand.wait_send())
    end_chunks(has_next, (onward,), range(2 * CHUNKS))
    end_chunks(gives, (give_low, give_high), range(CHUNKS))
    end_chunks(not_up, (give_low,), ACROSS)
    end_chunks(not_down, (give_high,), ACROSS)
    end_chunks(only_low, (give_low,), BESIDE)
    end_chunks(only_high, (give_high,), BESIDE)
    for there, copy, chunks in passes:
        end_chunks(there, (copy,), chunks)
    for there, _, _, copy in first_hops + second_hops:
        pl.when(there)(lambda copy=copy: copy.wait_send())

    for stage in range(3):
        for d in range(1, 4):
            sum_copy(*early, stage, 0, d, r).wait_send()
            sum_copy(*late, stage, 0, d, r).wait_send()


def apply_kernel(
    prev, z_hi, z_lo, plow, phigh, pot, w, r, basis_o, ritz_o, residual_o, out, out_sem, ritz_sem
):
    size = plow.shape[1]
    width = size // CHUNKS
    n = prev.shape[0]
    ritz = pltpu.make_async_copy(r, ritz_o, ritz_sem)
    ritz.start()

    def at(c):
        return pl.ds(pl.multiple_of(c * width, LANES), width)

    def writes(plane, c):
        where = at(plane * CHUNKS + c)
        return [
            pltpu.make_async_copy(out.at[plane, pl.ds(e * n, n)], dst.at[:, where], out_sem.at[plane, e])
            for e, dst in enumerate((basis_o, residual_o))
        ]

    w_hi, w_lo = split(w[...])
    both = jnp.concatenate([w_hi, w_lo], axis=0)

    @pl.loop(0, CHUNKS)
    def _(c):
        for plane in range(2):
            where = at(plane * CHUNKS + c)
            image_hi, image_lo = split(stencil(prev, plow, phigh, pot, plane, c, size, width))
            wide = jnp.dot(
                both, jnp.concatenate([z_hi[:, where], image_hi], axis=0), preferred_element_type=F32
            )
            narrow = jnp.dot(
                w_hi, jnp.concatenate([z_lo[:, where], image_lo], axis=0), preferred_element_type=F32
            )
            value = (wide[: 2 * n] + wide[2 * n :]) + narrow

            @pl.when(c > 0)
            def _():
                for copy in writes(plane, c - 1):
                    copy.wait()

            out[plane] = value
            for copy in writes(plane, c):
                copy.start()

    for plane in range(2):
        for copy in writes(plane, CHUNKS - 1):
            copy.wait()
    ritz.wait()


def solution(mesh):
    intervals, rows = mesh.shape["interval"], mesh.shape["rows"]

    def body(filtered, potential):
        x = filtered[0]
        n, cells = x.shape
        size = cells // 2
        width = size // CHUNKS
        pot = potential.reshape(1, cells)
        hbm = pl.BlockSpec(memory_space=pltpu.HBM)
        vmem = pl.BlockSpec(memory_space=pltpu.VMEM)
        whole = jax.ShapeDtypeStruct((n, cells), F32)
        plane = jax.ShapeDtypeStruct((n, size), F32)
        dma = pltpu.SemaphoreType.DMA

        def kernel(*refs):
            exchange_kernel(intervals, rows, *refs)

        stack = jax.ShapeDtypeStruct((3 * n, cells), BF16)
        prev, z_hi, z_lo, plow, phigh, w, r = pl.pallas_call(
            kernel,
            out_shape=(
                whole, stack, stack, plane, plane,
                jax.ShapeDtypeStruct((2 * n, 4 * n), F32),
                jax.ShapeDtypeStruct((n, n), F32),
            ),
            in_specs=[vmem, vmem],
            out_specs=(vmem,) * 7,
            scratch_shapes=[
                pltpu.VMEM((n, size), F32),
                pltpu.VMEM((n, size), F32),
                *[pltpu.VMEM((n, width), F32) for _ in range(4)],
                pltpu.VMEM((4 * n, 4 * n), F32),
                pltpu.VMEM((3, 4, n + n // 2, 2 * n), F32),
                pltpu.VMEM((n + n // 2, 2 * n), F32),
                pltpu.VMEM((n // 2, 2 * n), F32),
                pltpu.VMEM((3, 4, n // 2, 2 * n), F32),
                pltpu.VMEM((n // 2, 2 * n), F32),
                pltpu.VMEM((n // 2, 2 * n), F32),
                pltpu.VMEM((n, n), F32),
                dma((2 * CHUNKS,)), dma((2 * CHUNKS,)),
                dma((CHUNKS,)), dma((CHUNKS,)), dma((CHUNKS,)), dma((CHUNKS,)),
                dma((4,)), dma((4,)),
                dma((CHUNKS,)), dma((CHUNKS,)),
                dma((CHUNKS,)), dma((CHUNKS,)), dma((CHUNKS,)), dma((CHUNKS,)),
                dma((3, 4)), dma((3, 4)),
                dma, dma,
                dma((3, 4)), dma((3, 4)),
                dma, dma,
            ],
            compiler_params=pltpu.CompilerParams(
                collective_id=0, has_side_effects=True, vmem_limit_bytes=VMEM_EXCHANGE
            ),
            name="exchange",
        )(x, pot)
        basis, ritz, residual = pl.pallas_call(
            apply_kernel,
            out_shape=(whole, jax.ShapeDtypeStruct((n, n), F32), whole),
            in_specs=[vmem] * 8,
            out_specs=(hbm,) * 3,
            scratch_shapes=[pltpu.VMEM((2, 2 * n, width), F32), dma((2, 2)), dma],
            compiler_params=pltpu.CompilerParams(vmem_limit_bytes=VMEM_APPLY),
            name="apply",
        )(prev, z_hi, z_lo, plow, phigh, pot, w, r)
        return basis[None], ritz[None], residual[None]

    return jax.shard_map(
        body,
        mesh=mesh,
        in_specs=(P("interval", None, "rows"), P("rows", None, None)),
        out_specs=(
            P("interval", None, "rows"),
            P("interval", None, None),
            P("interval", None, "rows"),
        ),
        check_vma=False,
    )
```

```python
import functools

import jax
import jax.numpy as jnp
from jax import lax
from jax.experimental import pallas as pl
from jax.experimental.pallas import tpu as pltpu
from jax.sharding import PartitionSpec as P

MESH = pl.DeviceIdType.MESH
F32 = jnp.float32
BF16 = jnp.bfloat16

LANES = 128
VMEM_EXCHANGE, VMEM_APPLY = 16 * 2**20, 8 * 2**20
LAYER = 16
CHUNKS = 8
RELAYS_UP = {0: 3, 1: 7, 2: 10, 5: 14, 6: 13, 7: 11}
RELAYS_DOWN = {0: 12, 1: 8, 2: 5, 5: 1, 6: 2, 7: 10}
LANDING = 4
FIRST_CROSS, THEN_CROSS = (6, 5), (4, 2, 0, 1, 3, 7)
ACROSS, BESIDE = (2, 5, 7), (0, 1, 3, 4, 6)
NEAR, LAST = (0, 1, 2, 3, 4, 5, 6), (7,)
FIRST_ONWARD, NEXT_ONWARD = 2, 4
INVERT_AT = 5


def split(v):
    hi = v.astype(BF16)
    return hi, (v - hi.astype(F32)).astype(BF16)


def exact_dot(a, b, dims):
    return lax.dot_general(
        a, b, (dims, ((), ())), precision=lax.Precision.HIGHEST, preferred_element_type=F32
    )


def stencil(u, low, high, pot, plane, j, size, width):
    base = plane * size
    start = pl.multiple_of(base + j * width, LANES)
    c = u[:, pl.ds(start, width)]
    first = pl.multiple_of(jnp.maximum(start - LANES, base), LANES)
    last = pl.multiple_of(jnp.minimum(start + width, base + size - LANES), LANES)
    before = jnp.where(j > 0, u[:, pl.ds(first, LANES)], 0.0)
    after = jnp.where(j < size // width - 1, u[:, pl.ds(last, LANES)], 0.0)
    tiles = width // LANES
    part = [c[:, t * LANES : (t + 1) * LANES] for t in range(tiles)]
    around = [before, *part, after]
    lane = lax.broadcasted_iota(jnp.int32, part[0].shape, 1)
    other = u[:, pl.ds(pl.multiple_of((1 - plane) * size + j * width, LANES), width)]
    halo = (high if plane else low)[:, pl.ds(pl.multiple_of(j * width, LANES), width)]
    weight = 6.0 + pot[:, pl.ds(start, width)]
    out = []
    for t in range(tiles):
        cut = slice(t * LANES, (t + 1) * LANES)
        left = jnp.where(lane == 0, 0.0, pltpu.roll(part[t], 1, 1))
        right = jnp.where(lane == LANES - 1, 0.0, pltpu.roll(part[t], LANES - 1, 1))
        beside = (other[:, cut] + halo[:, cut]) + (around[t] + around[t + 2]) + (left + right)
        out.append(weight[:, cut] * part[t] - beside)
    return jnp.concatenate(out, axis=1)


def inverse_factor(square):
    n = square.shape[0]
    row = lax.broadcasted_iota(jnp.int32, (n, LANES), 0)
    lane = lax.broadcasted_iota(jnp.int32, (n, LANES), 1)
    t = jnp.where(lane < n, square, jnp.where(lane == row + n, 1.0, 0.0))
    rows = [t[b : b + 8] for b in range(0, n, 8)]
    shape = (8, LANES)
    place = lax.broadcasted_iota(jnp.int32, shape, 0)
    for k in range(0, n, 2):
        at, own = k % 8, rows[k // 8]
        top, under = own[at : at + 1, :], own[at + 1 : at + 2, :]
        one = 1.0 / own[at : at + 1, k : k + 1]
        ratio = own[at + 1 : at + 2, k : k + 1] * one
        under = under - top * ratio
        two = 1.0 / (own[at + 1 : at + 2, k + 1 : k + 2] - own[at : at + 1, k + 1 : k + 2] * ratio)
        scaled, scaled_under = top * one, under * two
        for b in range(k // 8, n // 8):
            first = jnp.broadcast_to(rows[b][:, k : k + 1], shape)
            second = jnp.broadcast_to(rows[b][:, k + 1 : k + 2], shape) - first * ratio
            if b == k // 8:
                first = jnp.where(place > at, first, 0.0)
                second = jnp.where(place > at + 1, second, 0.0)
            rows[b] = rows[b] - first * scaled - second * scaled_under
    t = jnp.concatenate(rows, axis=0)
    diagonal = jnp.sum(jnp.where(lane == row, t, 0.0), axis=1, keepdims=True)
    t = t * (1.0 / jnp.sqrt(diagonal))
    return pltpu.roll(t, LANES - n, 1)[:, :n]


def pack(upper, lower):
    lane = lax.broadcasted_iota(jnp.int32, upper.shape, 1)
    return jnp.where(lane < LANES // 2, upper, lower)


def unpack(packed):
    return jnp.concatenate([packed, pltpu.roll(packed, LANES // 2, 1)], axis=0)


def coefficients(own, total, inv_p, prior, wait_prior, w_out, r_out):
    n = total.shape[0] - own.shape[0]
    gram = unpack(own)[:, :n]
    g_pi, k_pi = total[:n, :n], pltpu.roll(total[:n], n, 1)[:, :n]
    k_own = unpack(total[n:])[:, :n]
    et = exact_dot(inv_p, g_pi, ((1,), (0,)))
    schur = gram - exact_dot(et, et, ((0,), (0,)))
    toward = exact_dot(et, inv_p, ((0,), (0,)))
    wide = jnp.concatenate([schur, jnp.zeros_like(schur)], axis=1)
    a = inverse_factor(wide)
    b = -exact_dot(a, toward, ((1,), (0,)))
    mixed = exact_dot(b, k_pi, ((1,), (0,)))
    ritz = exact_dot(exact_dot(a, k_own, ((1,), (0,))), a, ((1,), (1,)))
    ritz = ritz + exact_dot(mixed, a, ((1,), (1,))) + exact_dot(a, mixed, ((1,), (1,)))
    wait_prior()
    k_prior = unpack(prior[...])[:, :n]
    ritz = ritz + exact_dot(exact_dot(b, k_prior, ((1,), (0,))), b, ((1,), (1,)))
    r_out[...] = ritz
    ra = exact_dot(ritz, a, ((0,), (0,)))
    rb = exact_dot(ritz, b, ((0,), (0,)))
    zero = jnp.zeros_like(a)
    w_out[:n, :] = jnp.concatenate([a, b, zero, zero], axis=1)
    w_out[n:, :] = jnp.concatenate([-ra, -rb, a, b], axis=1)


def exchange_kernel(
    intervals, rows,
    x, pot,
    prev, z_hi, z_lo, plow_o, phigh_o, w_o, r_o,
    low, high, up_a, up_b, down_a, down_b, acc, sums, total, prior, early_sums, early_total, early_prior, inv_p,
    x_send, x_recv, up_send, down_send, low_recv, high_recv,
    relay_send, relay_recv, pass_up_send, pass_down_send, plow_send, phigh_send, plow_recv, phigh_recv,
    sum_send, sum_recv, prior_send, prior_recv,
    early_send, early_recv, early_prior_send, early_prior_recv,
):
    i, r = lax.axis_index("interval"), lax.axis_index("rows")
    layers = rows // LAYER
    layer, q = r // LAYER, r % LAYER
    qx, qy = q // 4, q % 4
    size = low.shape[1]
    width = size // CHUNKS

    def at(c):
        return pl.ds(pl.multiple_of(c * width, LANES), width)

    def remote(src, dst, send, recv, to_i, to_r):
        return pltpu.make_async_remote_copy(
            src_ref=src, dst_ref=dst, send_sem=send, recv_sem=recv,
            device_id=(to_i, to_r), device_id_type=MESH,
        )

    barrier = pltpu.get_barrier_semaphore()

    def greet(to_i, to_r):
        pl.semaphore_signal(barrier, inc=1, device_id=(to_i, to_r), device_id_type=MESH)

    for d in range(1, layers):
        greet(i, lax.rem(layer + d, layers) * LAYER + q)
    for d in range(1, LAYER):
        greet(i, layer * LAYER + lax.rem(q + d, LAYER))
    has_prev, has_next = i > 0, i < intervals - 1
    has_low, has_high = r > 0, r < rows - 1
    for there, to_i, to_r in (
        (has_prev, i - 1, r), (has_next, i + 1, r), (has_low, i, r - 1), (has_high, i, r + 1)
    ):
        pl.when(there)(lambda to_i=to_i, to_r=to_r: greet(to_i, to_r))
    neighbours = (
        has_prev.astype(jnp.int32) + has_next.astype(jnp.int32)
        + has_low.astype(jnp.int32) + has_high.astype(jnp.int32)
    )
    n = acc.shape[0] // 4
    early_acc = acc.at[pl.ds(0, 2 * n), pl.ds(0, 2 * n)]
    early_acc[...] = jnp.zeros((2 * n, 2 * n), F32)

    @pl.loop(0, 2 * CHUNKS)
    def _(c):
        both = jnp.concatenate(split(x[:, at(c)]), axis=0)
        early_acc[...] += lax.dot_general(
            both, both, (((1,), (1,)), ((), ())), preferred_element_type=F32
        )

    halves = early_acc[pl.ds(0, n), :] + pltpu.roll(early_acc[pl.ds(n, n), :], n, 1)
    own_gram = halves + pltpu.roll(halves, n, 1)
    own_gram = pack(own_gram[: n // 2], own_gram[n // 2 :])
    pl.semaphore_wait(barrier, layers - 1 + LAYER - 1 + neighbours)

    places = (
        (qy, lambda o: r - qy + o), (qx, lambda o: r - qx * 4 + o * 4), (layer, lambda o: o * LAYER + q)
    )

    def sum_copy(buffer, send, recv, stage, slot, d, to_r):
        return remote(
            buffer.at[stage, slot], buffer.at[stage, slot], send.at[stage, d], recv.at[stage, slot], i, to_r)

    def sum_start(buffer, send, recv, stage, value):
        mine, place = places[stage]
        buffer[stage, mine] = value
        for d in range(1, 4):
            sum_copy(buffer, send, recv, stage, mine, d, place(lax.rem(mine + d, 4))).start()

    def sum_end(buffer, send, recv, stage):
        mine, _ = places[stage]
        for d in range(1, 4):
            sum_copy(buffer, send, recv, stage, lax.rem(mine + d, 4), d, r).wait_recv()
        return (buffer[stage, 0] + buffer[stage, 1]) + (buffer[stage, 2] + buffer[stage, 3])

    early = (early_sums, early_send, early_recv)
    late = (sums, sum_send, sum_recv)

    def summed(stage, value):
        sum_start(*late, stage, value)
        return sum_end(*late, stage)

    sum_start(*early, 0, own_gram)

    last_of_layer, first_of_layer = q == LAYER - 1, q == 0
    cross_up = jnp.logical_and(last_of_layer, has_high)
    cross_down = jnp.logical_and(first_of_layer, has_low)
    plain_up = jnp.logical_not(last_of_layer)
    plain_down = jnp.logical_not(first_of_layer)
    spare = relay_send.at[0]

    def up_plain(c):
        return remote(x.at[:, at(CHUNKS + c)], low.at[:, at(c)], up_send.at[c], low_recv.at[c], i, r + 1)

    def down_plain(c):
        return remote(x.at[:, at(c)], high.at[:, at(c)], down_send.at[c], high_recv.at[c], i, r - 1)

    base = layer * LAYER

    def up_cross(c):
        if c not in RELAYS_UP and c != LANDING:
            return up_plain(c)
        return remote(
            x.at[:, at(CHUNKS + c)], up_a, up_send.at[c], relay_recv.at[0], i, base + RELAYS_UP.get(c, 0))

    def down_cross(c):
        if c not in RELAYS_DOWN and c != LANDING:
            return down_plain(c)
        return remote(
            x.at[:, at(c)], down_a, down_send.at[c], relay_recv.at[2],
            i, base + RELAYS_DOWN.get(c, LAYER - 1))

    def onward(c):
        return remote(x.at[:, at(c)], prev.at[:, at(c)], x_send.at[c], x_recv.at[c], i + 1, r)

    def start_chunks(there, copies, chunks):
        @pl.when(there)
        def _():
            for c in chunks:
                for copy in copies:
                    copy(c).start()

    def onward_low(c):
        return onward(c)

    def onward_high(c):
        return onward(CHUNKS + c)

    def start_onward(first, last):
        start_chunks(has_next, (onward_low, onward_high), range(first, last))

    all_of = lambda *terms: functools.reduce(jnp.logical_and, terms)
    start_onward(0, FIRST_ONWARD)
    start_chunks(cross_up, (up_cross,), FIRST_CROSS)
    start_chunks(cross_down, (down_cross,), FIRST_CROSS)
    start_chunks(qy < 3, (up_plain,), range(CHUNKS))
    start_chunks(qy > 0, (down_plain,), range(CHUNKS))
    own_gram = sum_end(*early, 0)
    sum_start(*early, 1, own_gram)
    start_chunks(cross_up, (up_cross,), THEN_CROSS)
    start_chunks(cross_down, (down_cross,), THEN_CROSS)
    start_chunks(all_of(qy == 3, plain_up), (up_plain,), range(CHUNKS))
    start_chunks(all_of(qy == 0, plain_down), (down_plain,), range(CHUNKS))
    own_gram = sum_end(*early, 1)
    sum_start(*early, 2, own_gram)
    start_onward(FIRST_ONWARD, NEXT_ONWARD)

    acc[...] = jnp.zeros_like(acc)

    @pl.when(jnp.logical_not(has_prev))
    def _():
        prev[...] = jnp.zeros_like(prev)

    @pl.when(jnp.logical_not(has_low))
    def _():
        low[...] = jnp.zeros_like(low)

    @pl.when(jnp.logical_not(has_high))
    def _():
        high[...] = jnp.zeros_like(high)

    def role(table):
        chunk, first = jnp.int32(0), jnp.bool_(False)
        for c, of in table.items():
            chunk = chunk + jnp.where(q == of, c, 0)
            first = jnp.logical_or(first, q == of)
        return chunk, first

    up_chunk, up_relay = role(RELAYS_UP)
    down_chunk, down_relay = role(RELAYS_DOWN)
    above, below = layer < layers - 1, layer > 0
    first_hops = (
        (jnp.logical_and(up_relay, above), 0, up_a, remote(
            up_a, up_b, relay_send.at[0], relay_recv.at[1], i, r + LAYER)),
        (jnp.logical_and(down_relay, below), 2, down_a, remote(
            down_a, down_b, relay_send.at[2], relay_recv.at[3], i, r - LAYER)),
        (jnp.logical_and(first_of_layer, above), 0, up_a, remote(
            up_a, low.at[:, at(LANDING)], relay_send.at[0], low_recv.at[LANDING], i, r + LAYER)),
        (jnp.logical_and(last_of_layer, below), 2, down_a, remote(
            down_a, high.at[:, at(LANDING)], relay_send.at[2], high_recv.at[LANDING], i, r - LAYER)),
    )
    second_hops = (
        (jnp.logical_and(up_relay, below), 1, up_b, remote(
            up_b, low.at[:, at(up_chunk)], relay_send.at[1], low_recv.at[up_chunk], i, base)),
        (jnp.logical_and(down_relay, above), 3, down_b, remote(
            down_b, high.at[:, at(down_chunk)], relay_send.at[3], high_recv.at[down_chunk],
            i, base + LAYER - 1)),
    )

    def relay(hops):
        for there, slot, buffer, copy in hops:
            @pl.when(there)
            def _(slot=slot, buffer=buffer, copy=copy):
                remote(buffer, buffer, spare, relay_recv.at[slot], i, r).wait_recv()
                copy.start()

    relay(first_hops)
    start_onward(NEXT_ONWARD, CHUNKS)
    relay(second_hops)
    early_total[...] = sum_end(*early, 2)
    early_hand = remote(early_total, early_prior, early_prior_send, early_prior_recv, i + 1, r)
    pl.when(has_next)(lambda: early_hand.start())

    @pl.when(jnp.logical_not(has_prev))
    def _():
        row = lax.broadcasted_iota(jnp.int32, early_prior.shape, 0)
        lane = lax.broadcasted_iota(jnp.int32, early_prior.shape, 1)
        early_prior[...] = jnp.where(lax.rem(lane, n) == row + n // 2 * (lane // n), 1.0, 0.0)
        prior[...] = jnp.zeros_like(prior)


    gives = lax.rem(i, 2) == 0
    across = jnp.logical_and(has_next, jnp.logical_not(gives))

    def give_low(c):
        return remote(low.at[:, at(c)], plow_o.at[:, at(c)], plow_send.at[c], plow_recv.at[c], i + 1, r)

    def give_high(c):
        return remote(high.at[:, at(c)], phigh_o.at[:, at(c)], phigh_send.at[c], phigh_recv.at[c], i + 1, r)

    lone = jnp.logical_and(has_prev, gives)

    def invert():
        pl.when(has_prev)(lambda: early_hand.wait_recv())
        inv_p[...] = inverse_factor(unpack(early_prior[...]))

    crossed = jnp.logical_or(cross_up, cross_down).astype(jnp.int32)

    @pl.loop(0, CHUNKS)
    def _(step):
        c = lax.rem(step + crossed, CHUNKS)
        pl.when(jnp.logical_and(step == INVERT_AT, jnp.logical_not(lone)))(invert)

        @pl.when(has_prev)
        def _():
            onward(c).wait_recv()
            onward(CHUNKS + c).wait_recv()

        @pl.when(has_low)
        def _():
            up_plain(c).wait_recv()

        @pl.when(has_high)
        def _():
            down_plain(c).wait_recv()

        @pl.when(gives)
        def _():
            give_low(c).start()
            give_high(c).start()

        for plane in range(2):
            mine = x[:, at(plane * CHUNKS + c)]
            image = stencil(x, low, high, pot, plane, c, size, width)
            theirs = prev[:, at(plane * CHUNKS + c)]
            mine_hi, mine_lo = split(mine)
            image_hi, image_lo = split(image)
            theirs_hi, theirs_lo = split(theirs)
            where = at(plane * CHUNKS + c)
            z_hi[:, where] = jnp.concatenate([mine_hi, theirs_hi, image_hi], axis=0)
            z_lo[:, where] = jnp.concatenate([mine_lo, theirs_lo, image_lo], axis=0)
            left = jnp.concatenate([mine_hi, theirs_hi, mine_lo, theirs_lo], axis=0)
            right = jnp.concatenate([mine_hi, image_hi, mine_lo, image_lo], axis=0)
            acc[...] += lax.dot_general(
                left, right, (((1,), (1,)), ((), ())), preferred_element_type=F32
            )

    half = acc.shape[0] // 2
    partial = acc[:half, :half] + acc[half:, half:] + (acc[:half, half:] + acc[half:, :half])
    square = pltpu.roll(partial[: n // 2], n, 1)
    partial = jnp.concatenate([partial[n:], pack(square, partial[n // 2 : n])], axis=0)

    def pass_up(c):
        return remote(
            prev.at[:, at(CHUNKS + c)], plow_o.at[:, at(c)], pass_up_send.at[c], plow_recv.at[c], i, r + 1)

    def pass_down(c):
        return remote(
            prev.at[:, at(c)], phigh_o.at[:, at(c)], pass_down_send.at[c], phigh_recv.at[c], i, r - 1)

    def none_low(c):
        return pltpu.make_async_copy(prev.at[:, at(c)], plow_o.at[:, at(c)], plow_recv.at[c])

    def none_high(c):
        return pltpu.make_async_copy(prev.at[:, at(c)], phigh_o.at[:, at(c)], phigh_recv.at[c])

    def own_low(c):
        return pltpu.make_async_copy(low.at[:, at(c)], plow_o.at[:, at(c)], plow_recv.at[c])

    def own_high(c):
        return pltpu.make_async_copy(high.at[:, at(c)], phigh_o.at[:, at(c)], phigh_recv.at[c])

    start_chunks(jnp.logical_not(has_prev), (none_low, none_high), range(CHUNKS))
    start_chunks(all_of(lone, jnp.logical_not(has_low)), (own_low,), BESIDE)
    start_chunks(all_of(lone, jnp.logical_not(has_high)), (own_high,), BESIDE)
    passes = (
        (all_of(lone, qy < 3), pass_up, NEAR),
        (all_of(lone, q == LAYER - 2, above), pass_up, LAST),
        (all_of(lone, qy > 0), pass_down, NEAR),
        (all_of(lone, q == 1, below), pass_down, LAST),
        (all_of(lone, qy == 3, plain_up), pass_up, BESIDE),
        (all_of(lone, qy == 0, plain_down), pass_down, BESIDE),
    )
    only_high, only_low = jnp.logical_and(across, cross_up), jnp.logical_and(across, cross_down)
    not_up = jnp.logical_and(across, jnp.logical_not(cross_up))
    not_down = jnp.logical_and(across, jnp.logical_not(cross_down))
    gifts = (
        ((only_low, give_low, NEAR[:4]), (only_high, give_high, NEAR[:4])),
        (
            (only_low, give_low, NEAR[4:5]),
            (only_high, give_high, NEAR[4:5]),
            (all_of(not_up, not_down, qy == 0), give_low, ACROSS[:1]),
            (all_of(not_up, not_down, qy == 3), give_high, ACROSS[:1]),
            (all_of(not_up, qy > 0), give_low, LAST),
            (all_of(not_down, qy < 3), give_high, LAST),
        ),
        (
            (only_low, give_low, NEAR[5:] + LAST),
            (only_high, give_high, NEAR[5:] + LAST),
            (all_of(not_up, not_down, qy == 0), give_low, ACROSS[1:]),
            (all_of(not_up, not_down, qy == 3), give_high, ACROSS[1:]),
        ),
    )

    def start_gifts(part):
        for there, copy, chunks in gifts[part]:
            start_chunks(there, (copy,), chunks)

    sum_start(*late, 0, partial)
    for there, copy, chunks in passes[:4]:
        start_chunks(there, (copy,), chunks)
    start_gifts(0)
    pl.when(lone)(invert)
    partial = sum_end(*late, 0)
    partial = summed(1, partial)
    for there, copy, chunks in passes[4:]:
        start_chunks(there, (copy,), chunks)
    sum_start(*late, 2, partial)
    start_gifts(1)
    total[...] = sum_end(*late, 2)
    hand = remote(total.at[pl.ds(n, n // 2)], prior, prior_send, prior_recv, i + 1, r)
    pl.when(has_next)(lambda: hand.start())
    start_gifts(2)
    wait_prior = lambda: pl.when(has_prev)(lambda: hand.wait_recv())
    coefficients(early_total[...], total[...], inv_p[...], prior, wait_prior, w_o, r_o)

    for c in range(CHUNKS):
        give_low(c).wait_recv()
        give_high(c).wait_recv()

    def end_chunks(there, copies, chunks):
        @pl.when(there)
        def _():
            for c in chunks:
                for copy in copies:
                    copy(c).wait_send()

    end_chunks(has_high, (up_plain,), range(CHUNKS))
    end_chunks(has_low, (down_plain,), range(CHUNKS))
    pl.when(has_next)(lambda: hand.wait_send())
    pl.when(has_next)(lambda: early_hand.wait_send())
    end_chunks(has_next, (onward,), range(2 * CHUNKS))
    end_chunks(gives, (give_low, give_high), range(CHUNKS))
    for there, copy, chunks in passes + gifts[0] + gifts[1] + gifts[2]:
        end_chunks(there, (copy,), chunks)
    for there, _, _, copy in first_hops + second_hops:
        pl.when(there)(lambda copy=copy: copy.wait_send())

    for stage in range(3):
        for d in range(1, 4):
            sum_copy(*early, stage, 0, d, r).wait_send()
            sum_copy(*late, stage, 0, d, r).wait_send()


def apply_kernel(
    prev, z_hi, z_lo, plow, phigh, pot, w, r, basis_o, ritz_o, residual_o, out, out_sem, ritz_sem
):
    size = plow.shape[1]
    width = size // CHUNKS
    n = prev.shape[0]
    ritz = pltpu.make_async_copy(r, ritz_o, ritz_sem)
    ritz.start()

    def at(c):
        return pl.ds(pl.multiple_of(c * width, LANES), width)

    def writes(plane, c):
        where = at(plane * CHUNKS + c)
        return [
            pltpu.make_async_copy(out.at[plane, pl.ds(e * n, n)], dst.at[:, where], out_sem.at[plane, e])
            for e, dst in enumerate((basis_o, residual_o))
        ]

    w_hi, w_lo = split(w[...])
    both = jnp.concatenate([w_hi, w_lo], axis=0)

    @pl.loop(0, CHUNKS)
    def _(c):
        for plane in range(2):
            where = at(plane * CHUNKS + c)
            image_hi, image_lo = split(stencil(prev, plow, phigh, pot, plane, c, size, width))
            wide = jnp.dot(
                both, jnp.concatenate([z_hi[:, where], image_hi], axis=0), preferred_element_type=F32
            )
            narrow = jnp.dot(
                w_hi, jnp.concatenate([z_lo[:, where], image_lo], axis=0), preferred_element_type=F32
            )
            value = (wide[: 2 * n] + wide[2 * n :]) + narrow

            @pl.when(c > 0)
            def _():
                for copy in writes(plane, c - 1):
                    copy.wait()

            out[plane] = value
            for copy in writes(plane, c):
                copy.start()

    for plane in range(2):
        for copy in writes(plane, CHUNKS - 1):
            copy.wait()
    ritz.wait()


def solution(mesh):
    intervals, rows = mesh.shape["interval"], mesh.shape["rows"]

    def body(filtered, potential):
        x = filtered[0]
        n, cells = x.shape
        size = cells // 2
        width = size // CHUNKS
        pot = potential.reshape(1, cells)
        hbm = pl.BlockSpec(memory_space=pltpu.HBM)
        vmem = pl.BlockSpec(memory_space=pltpu.VMEM)
        whole = jax.ShapeDtypeStruct((n, cells), F32)
        plane = jax.ShapeDtypeStruct((n, size), F32)
        dma = pltpu.SemaphoreType.DMA

        def kernel(*refs):
            exchange_kernel(intervals, rows, *refs)

        stack = jax.ShapeDtypeStruct((3 * n, cells), BF16)
        prev, z_hi, z_lo, plow, phigh, w, r = pl.pallas_call(
            kernel,
            out_shape=(
                whole, stack, stack, plane, plane,
                jax.ShapeDtypeStruct((2 * n, 4 * n), F32),
                jax.ShapeDtypeStruct((n, n), F32),
            ),
            in_specs=[vmem, vmem],
            out_specs=(vmem,) * 7,
            scratch_shapes=[
                pltpu.VMEM((n, size), F32),
                pltpu.VMEM((n, size), F32),
                *[pltpu.VMEM((n, width), F32) for _ in range(4)],
                pltpu.VMEM((4 * n, 4 * n), F32),
                pltpu.VMEM((3, 4, n + n // 2, 2 * n), F32),
                pltpu.VMEM((n + n // 2, 2 * n), F32),
                pltpu.VMEM((n // 2, 2 * n), F32),
                pltpu.VMEM((3, 4, n // 2, 2 * n), F32),
                pltpu.VMEM((n // 2, 2 * n), F32),
                pltpu.VMEM((n // 2, 2 * n), F32),
                pltpu.VMEM((n, n), F32),
                dma((2 * CHUNKS,)), dma((2 * CHUNKS,)),
                dma((CHUNKS,)), dma((CHUNKS,)), dma((CHUNKS,)), dma((CHUNKS,)),
                dma((4,)), dma((4,)),
                dma((CHUNKS,)), dma((CHUNKS,)),
                dma((CHUNKS,)), dma((CHUNKS,)), dma((CHUNKS,)), dma((CHUNKS,)),
                dma((3, 4)), dma((3, 4)),
                dma, dma,
                dma((3, 4)), dma((3, 4)),
                dma, dma,
            ],
            compiler_params=pltpu.CompilerParams(
                collective_id=0, has_side_effects=True, vmem_limit_bytes=VMEM_EXCHANGE
            ),
            name="exchange",
        )(x, pot)
        basis, ritz, residual = pl.pallas_call(
            apply_kernel,
            out_shape=(whole, jax.ShapeDtypeStruct((n, n), F32), whole),
            in_specs=[vmem] * 8,
            out_specs=(hbm,) * 3,
            scratch_shapes=[pltpu.VMEM((2, 2 * n, width), F32), dma((2, 2)), dma],
            compiler_params=pltpu.CompilerParams(vmem_limit_bytes=VMEM_APPLY),
            name="apply",
        )(prev, z_hi, z_lo, plow, phigh, pot, w, r)
        return basis[None], ritz[None], residual[None]

    return jax.shard_map(
        body,
        mesh=mesh,
        in_specs=(P("interval", None, "rows"), P("rows", None, None)),
        out_specs=(
            P("interval", None, "rows"),
            P("interval", None, None),
            P("interval", None, "rows"),
        ),
        check_vma=False,
    )
```

```python
import functools

import jax
import jax.numpy as jnp
from jax import lax
from jax.experimental import pallas as pl
from jax.experimental.pallas import tpu as pltpu
from jax.sharding import PartitionSpec as P

MESH = pl.DeviceIdType.MESH
F32 = jnp.float32
BF16 = jnp.bfloat16

LANES = 128
VMEM_EXCHANGE, VMEM_APPLY = 16 * 2**20, 8 * 2**20
LAYER = 16
CHUNKS = 8
RELAYS_UP = {0: 3, 1: 7, 2: 10, 5: 14, 6: 13, 7: 11}
RELAYS_DOWN = {0: 12, 1: 8, 2: 5, 5: 1, 6: 2, 7: 10}
LANDING = 4
FIRST_CROSS, THEN_CROSS = (6, 5), (4, 2, 0, 1, 3, 7)
ACROSS, BESIDE = (2, 5, 7), (0, 1, 3, 4, 6)
NEAR, LAST = (0, 1, 2, 3, 4, 5, 6), (7,)
FIRST_ONWARD, NEXT_ONWARD = 2, 4
INVERT_AT = 5


def split(v):
    hi = v.astype(BF16)
    return hi, (v - hi.astype(F32)).astype(BF16)


def exact_dot(a, b, dims):
    return lax.dot_general(
        a, b, (dims, ((), ())), precision=lax.Precision.HIGHEST, preferred_element_type=F32
    )


def stencil(u, low, high, pot, plane, j, size, width):
    base = plane * size
    start = pl.multiple_of(base + j * width, LANES)
    c = u[:, pl.ds(start, width)]
    first = pl.multiple_of(jnp.maximum(start - LANES, base), LANES)
    last = pl.multiple_of(jnp.minimum(start + width, base + size - LANES), LANES)
    before = jnp.where(j > 0, u[:, pl.ds(first, LANES)], 0.0)
    after = jnp.where(j < size // width - 1, u[:, pl.ds(last, LANES)], 0.0)
    tiles = width // LANES
    part = [c[:, t * LANES : (t + 1) * LANES] for t in range(tiles)]
    around = [before, *part, after]
    lane = lax.broadcasted_iota(jnp.int32, part[0].shape, 1)
    other = u[:, pl.ds(pl.multiple_of((1 - plane) * size + j * width, LANES), width)]
    halo = (high if plane else low)[:, pl.ds(pl.multiple_of(j * width, LANES), width)]
    weight = 6.0 + pot[:, pl.ds(start, width)]
    out = []
    for t in range(tiles):
        cut = slice(t * LANES, (t + 1) * LANES)
        left = jnp.where(lane == 0, 0.0, pltpu.roll(part[t], 1, 1))
        right = jnp.where(lane == LANES - 1, 0.0, pltpu.roll(part[t], LANES - 1, 1))
        beside = (other[:, cut] + halo[:, cut]) + (around[t] + around[t + 2]) + (left + right)
        out.append(weight[:, cut] * part[t] - beside)
    return jnp.concatenate(out, axis=1)


def inverse_factor(square):
    n = square.shape[0]
    row = lax.broadcasted_iota(jnp.int32, (n, LANES), 0)
    lane = lax.broadcasted_iota(jnp.int32, (n, LANES), 1)
    t = jnp.where(lane < n, square, jnp.where(lane == row + n, 1.0, 0.0))
    rows = [t[b : b + 8] for b in range(0, n, 8)]
    shape = (8, LANES)
    place = lax.broadcasted_iota(jnp.int32, shape, 0)
    for k in range(0, n, 2):
        at, own = k % 8, rows[k // 8]
        top, under = own[at : at + 1, :], own[at + 1 : at + 2, :]
        one = 1.0 / own[at : at + 1, k : k + 1]
        ratio = own[at + 1 : at + 2, k : k + 1] * one
        under = under - top * ratio
        two = 1.0 / (own[at + 1 : at + 2, k + 1 : k + 2] - own[at : at + 1, k + 1 : k + 2] * ratio)
        scaled, scaled_under = top * one, under * two
        for b in range(k // 8, n // 8):
            first = jnp.broadcast_to(rows[b][:, k : k + 1], shape)
            second = jnp.broadcast_to(rows[b][:, k + 1 : k + 2], shape) - first * ratio
            if b == k // 8:
                first = jnp.where(place > at, first, 0.0)
                second = jnp.where(place > at + 1, second, 0.0)
            rows[b] = rows[b] - first * scaled - second * scaled_under
    t = jnp.concatenate(rows, axis=0)
    diagonal = jnp.sum(jnp.where(lane == row, t, 0.0), axis=1, keepdims=True)
    t = t * (1.0 / jnp.sqrt(diagonal))
    return pltpu.roll(t, LANES - n, 1)[:, :n]


def pack(upper, lower):
    lane = lax.broadcasted_iota(jnp.int32, upper.shape, 1)
    return jnp.where(lane < LANES // 2, upper, lower)


def unpack(packed):
    return jnp.concatenate([packed, pltpu.roll(packed, LANES // 2, 1)], axis=0)


def coefficients(own, total, inv_p, prior, wait_prior, w_out, r_out):
    n = total.shape[0] - own.shape[0]
    gram = unpack(own)[:, :n]
    g_pi, k_pi = total[:n, :n], pltpu.roll(total[:n], n, 1)[:, :n]
    k_own = unpack(total[n:])[:, :n]
    et = exact_dot(inv_p, g_pi, ((1,), (0,)))
    schur = gram - exact_dot(et, et, ((0,), (0,)))
    toward = exact_dot(et, inv_p, ((0,), (0,)))
    wide = jnp.concatenate([schur, jnp.zeros_like(schur)], axis=1)
    a = inverse_factor(wide)
    b = -exact_dot(a, toward, ((1,), (0,)))
    mixed = exact_dot(b, k_pi, ((1,), (0,)))
    ritz = exact_dot(exact_dot(a, k_own, ((1,), (0,))), a, ((1,), (1,)))
    ritz = ritz + exact_dot(mixed, a, ((1,), (1,))) + exact_dot(a, mixed, ((1,), (1,)))
    wait_prior()
    k_prior = unpack(prior[...])[:, :n]
    ritz = ritz + exact_dot(exact_dot(b, k_prior, ((1,), (0,))), b, ((1,), (1,)))
    r_out[...] = ritz
    ra = exact_dot(ritz, a, ((0,), (0,)))
    rb = exact_dot(ritz, b, ((0,), (0,)))
    zero = jnp.zeros_like(a)
    w_out[:n, :] = jnp.concatenate([a, b, zero, zero], axis=1)
    w_out[n:, :] = jnp.concatenate([-ra, -rb, a, b], axis=1)


def exchange_kernel(
    intervals, rows,
    x, pot,
    prev, z_hi, z_lo, plow_o, phigh_o, w_o, r_o,
    low, high, up_a, up_b, down_a, down_b, acc, sums, total, prior, early_sums, early_total, early_prior, inv_p,
    x_send, x_recv, up_send, down_send, low_recv, high_recv,
    relay_send, relay_recv, pass_up_send, pass_down_send, plow_send, phigh_send, plow_recv, phigh_recv,
    sum_send, sum_recv, prior_send, prior_recv,
    early_send, early_recv, early_prior_send, early_prior_recv,
):
    i, r = lax.axis_index("interval"), lax.axis_index("rows")
    layers = rows // LAYER
    layer, q = r // LAYER, r % LAYER
    qx, qy = q // 4, q % 4
    size = low.shape[1]
    width = size // CHUNKS

    def at(c):
        return pl.ds(pl.multiple_of(c * width, LANES), width)

    def remote(src, dst, send, recv, to_i, to_r):
        return pltpu.make_async_remote_copy(
            src_ref=src, dst_ref=dst, send_sem=send, recv_sem=recv,
            device_id=(to_i, to_r), device_id_type=MESH,
        )

    barrier = pltpu.get_barrier_semaphore()

    def greet(to_i, to_r):
        pl.semaphore_signal(barrier, inc=1, device_id=(to_i, to_r), device_id_type=MESH)

    for d in range(1, layers):
        greet(i, lax.rem(layer + d, layers) * LAYER + q)
    for d in range(1, LAYER):
        greet(i, layer * LAYER + lax.rem(q + d, LAYER))
    has_prev, has_next = i > 0, i < intervals - 1
    has_low, has_high = r > 0, r < rows - 1
    for there, to_i, to_r in (
        (has_prev, i - 1, r), (has_next, i + 1, r), (has_low, i, r - 1), (has_high, i, r + 1)
    ):
        pl.when(there)(lambda to_i=to_i, to_r=to_r: greet(to_i, to_r))
    neighbours = (
        has_prev.astype(jnp.int32) + has_next.astype(jnp.int32)
        + has_low.astype(jnp.int32) + has_high.astype(jnp.int32)
    )
    n = acc.shape[0] // 4
    early_acc = acc.at[pl.ds(0, 2 * n), pl.ds(0, 2 * n)]
    early_acc[...] = jnp.zeros((2 * n, 2 * n), F32)

    @pl.loop(0, 2 * CHUNKS)
    def _(c):
        both = jnp.concatenate(split(x[:, at(c)]), axis=0)
        early_acc[...] += lax.dot_general(
            both, both, (((1,), (1,)), ((), ())), preferred_element_type=F32
        )

    halves = early_acc[pl.ds(0, n), :] + pltpu.roll(early_acc[pl.ds(n, n), :], n, 1)
    own_gram = halves + pltpu.roll(halves, n, 1)
    own_gram = pack(own_gram[: n // 2], own_gram[n // 2 :])
    pl.semaphore_wait(barrier, layers - 1 + LAYER - 1 + neighbours)

    places = (
        (qy, lambda o: r - qy + o), (qx, lambda o: r - qx * 4 + o * 4), (layer, lambda o: o * LAYER + q)
    )

    def sum_copy(buffer, send, recv, stage, slot, d, to_r):
        return remote(
            buffer.at[stage, slot], buffer.at[stage, slot], send.at[stage, d], recv.at[stage, slot], i, to_r)

    def sum_start(buffer, send, recv, stage, value):
        mine, place = places[stage]
        buffer[stage, mine] = value
        for d in range(1, 4):
            sum_copy(buffer, send, recv, stage, mine, d, place(lax.rem(mine + d, 4))).start()

    def sum_end(buffer, send, recv, stage):
        mine, _ = places[stage]
        for d in range(1, 4):
            sum_copy(buffer, send, recv, stage, lax.rem(mine + d, 4), d, r).wait_recv()
        return (buffer[stage, 0] + buffer[stage, 1]) + (buffer[stage, 2] + buffer[stage, 3])

    early = (early_sums, early_send, early_recv)
    late = (sums, sum_send, sum_recv)

    sum_start(*early, 0, own_gram)

    last_of_layer, first_of_layer = q == LAYER - 1, q == 0
    cross_up = jnp.logical_and(last_of_layer, has_high)
    cross_down = jnp.logical_and(first_of_layer, has_low)
    plain_up = jnp.logical_not(last_of_layer)
    plain_down = jnp.logical_not(first_of_layer)
    spare = relay_send.at[0]

    def up_plain(c):
        return remote(x.at[:, at(CHUNKS + c)], low.at[:, at(c)], up_send.at[c], low_recv.at[c], i, r + 1)

    def down_plain(c):
        return remote(x.at[:, at(c)], high.at[:, at(c)], down_send.at[c], high_recv.at[c], i, r - 1)

    base = layer * LAYER

    def up_cross(c):
        if c not in RELAYS_UP and c != LANDING:
            return up_plain(c)
        return remote(
            x.at[:, at(CHUNKS + c)], up_a, up_send.at[c], relay_recv.at[0], i, base + RELAYS_UP.get(c, 0))

    def down_cross(c):
        if c not in RELAYS_DOWN and c != LANDING:
            return down_plain(c)
        return remote(
            x.at[:, at(c)], down_a, down_send.at[c], relay_recv.at[2],
            i, base + RELAYS_DOWN.get(c, LAYER - 1))

    def onward(c):
        return remote(x.at[:, at(c)], prev.at[:, at(c)], x_send.at[c], x_recv.at[c], i + 1, r)

    def start_chunks(there, copies, chunks):
        @pl.when(there)
        def _():
            for c in chunks:
                for copy in copies:
                    copy(c).start()

    def onward_low(c):
        return onward(c)

    def onward_high(c):
        return onward(CHUNKS + c)

    def start_onward(first, last):
        start_chunks(has_next, (onward_low, onward_high), range(first, last))

    all_of = lambda *terms: functools.reduce(jnp.logical_and, terms)
    start_onward(0, FIRST_ONWARD)
    start_chunks(cross_up, (up_cross,), FIRST_CROSS)
    start_chunks(cross_down, (down_cross,), FIRST_CROSS)
    start_chunks(qy < 3, (up_plain,), range(CHUNKS))
    start_chunks(qy > 0, (down_plain,), range(CHUNKS))
    own_gram = sum_end(*early, 0)
    sum_start(*early, 1, own_gram)
    start_chunks(cross_up, (up_cross,), THEN_CROSS)
    start_chunks(cross_down, (down_cross,), THEN_CROSS)
    start_chunks(all_of(qy == 3, plain_up), (up_plain,), range(CHUNKS))
    start_chunks(all_of(qy == 0, plain_down), (down_plain,), range(CHUNKS))
    own_gram = sum_end(*early, 1)
    sum_start(*early, 2, own_gram)
    start_onward(FIRST_ONWARD, NEXT_ONWARD)

    acc[...] = jnp.zeros_like(acc)

    @pl.when(jnp.logical_not(has_prev))
    def _():
        prev[...] = jnp.zeros_like(prev)

    @pl.when(jnp.logical_not(has_low))
    def _():
        low[...] = jnp.zeros_like(low)

    @pl.when(jnp.logical_not(has_high))
    def _():
        high[...] = jnp.zeros_like(high)

    def role(table):
        chunk, first = jnp.int32(0), jnp.bool_(False)
        for c, of in table.items():
            chunk = chunk + jnp.where(q == of, c, 0)
            first = jnp.logical_or(first, q == of)
        return chunk, first

    up_chunk, up_relay = role(RELAYS_UP)
    down_chunk, down_relay = role(RELAYS_DOWN)
    above, below = layer < layers - 1, layer > 0
    first_hops = (
        (jnp.logical_and(up_relay, above), 0, up_a, remote(
            up_a, up_b, relay_send.at[0], relay_recv.at[1], i, r + LAYER)),
        (jnp.logical_and(down_relay, below), 2, down_a, remote(
            down_a, down_b, relay_send.at[2], relay_recv.at[3], i, r - LAYER)),
        (jnp.logical_and(first_of_layer, above), 0, up_a, remote(
            up_a, low.at[:, at(LANDING)], relay_send.at[0], low_recv.at[LANDING], i, r + LAYER)),
        (jnp.logical_and(last_of_layer, below), 2, down_a, remote(
            down_a, high.at[:, at(LANDING)], relay_send.at[2], high_recv.at[LANDING], i, r - LAYER)),
    )
    second_hops = (
        (jnp.logical_and(up_relay, below), 1, up_b, remote(
            up_b, low.at[:, at(up_chunk)], relay_send.at[1], low_recv.at[up_chunk], i, base)),
        (jnp.logical_and(down_relay, above), 3, down_b, remote(
            down_b, high.at[:, at(down_chunk)], relay_send.at[3], high_recv.at[down_chunk],
            i, base + LAYER - 1)),
    )

    def relay(hops):
        for there, slot, buffer, copy in hops:
            @pl.when(there)
            def _(slot=slot, buffer=buffer, copy=copy):
                remote(buffer, buffer, spare, relay_recv.at[slot], i, r).wait_recv()
                copy.start()

    relay(first_hops)
    start_onward(NEXT_ONWARD, CHUNKS)
    relay(second_hops)
    early_total[...] = sum_end(*early, 2)
    early_hand = remote(early_total, early_prior, early_prior_send, early_prior_recv, i + 1, r)
    pl.when(has_next)(lambda: early_hand.start())

    @pl.when(jnp.logical_not(has_prev))
    def _():
        row = lax.broadcasted_iota(jnp.int32, early_prior.shape, 0)
        lane = lax.broadcasted_iota(jnp.int32, early_prior.shape, 1)
        early_prior[...] = jnp.where(lax.rem(lane, n) == row + n // 2 * (lane // n), 1.0, 0.0)
        prior[...] = jnp.zeros_like(prior)


    gives = lax.rem(i, 2) == 0
    across = jnp.logical_and(has_next, jnp.logical_not(gives))

    def give_low(c):
        return remote(low.at[:, at(c)], plow_o.at[:, at(c)], plow_send.at[c], plow_recv.at[c], i + 1, r)

    def give_high(c):
        return remote(high.at[:, at(c)], phigh_o.at[:, at(c)], phigh_send.at[c], phigh_recv.at[c], i + 1, r)

    lone = jnp.logical_and(has_prev, gives)

    def invert():
        pl.when(has_prev)(lambda: early_hand.wait_recv())
        inv_p[...] = inverse_factor(unpack(early_prior[...]))

    crossed = jnp.logical_or(cross_up, cross_down).astype(jnp.int32)

    @pl.loop(0, CHUNKS)
    def _(step):
        c = lax.rem(step + crossed, CHUNKS)
        pl.when(jnp.logical_and(step == INVERT_AT, jnp.logical_not(lone)))(invert)

        @pl.when(has_prev)
        def _():
            onward(c).wait_recv()
            onward(CHUNKS + c).wait_recv()

        @pl.when(has_low)
        def _():
            up_plain(c).wait_recv()

        @pl.when(has_high)
        def _():
            down_plain(c).wait_recv()

        @pl.when(gives)
        def _():
            give_low(c).start()
            give_high(c).start()

        for plane in range(2):
            mine = x[:, at(plane * CHUNKS + c)]
            image = stencil(x, low, high, pot, plane, c, size, width)
            theirs = prev[:, at(plane * CHUNKS + c)]
            mine_hi, mine_lo = split(mine)
            image_hi, image_lo = split(image)
            theirs_hi, theirs_lo = split(theirs)
            where = at(plane * CHUNKS + c)
            z_hi[:, where] = jnp.concatenate([mine_hi, theirs_hi, image_hi], axis=0)
            z_lo[:, where] = jnp.concatenate([mine_lo, theirs_lo, image_lo], axis=0)
            left = jnp.concatenate([mine_hi, theirs_hi, mine_lo, theirs_lo], axis=0)
            right = jnp.concatenate([mine_hi, image_hi, mine_lo, image_lo], axis=0)
            acc[...] += lax.dot_general(
                left, right, (((1,), (1,)), ((), ())), preferred_element_type=F32
            )

    half = acc.shape[0] // 2
    partial = acc[:half, :half] + acc[half:, half:] + (acc[:half, half:] + acc[half:, :half])
    square = pltpu.roll(partial[: n // 2], n, 1)
    partial = jnp.concatenate([partial[n:], pack(square, partial[n // 2 : n])], axis=0)

    def pass_up(c):
        return remote(
            prev.at[:, at(CHUNKS + c)], plow_o.at[:, at(c)], pass_up_send.at[c], plow_recv.at[c], i, r + 1)

    def pass_down(c):
        return remote(
            prev.at[:, at(c)], phigh_o.at[:, at(c)], pass_down_send.at[c], phigh_recv.at[c], i, r - 1)

    def none_low(c):
        return pltpu.make_async_copy(prev.at[:, at(c)], plow_o.at[:, at(c)], plow_recv.at[c])

    def none_high(c):
        return pltpu.make_async_copy(prev.at[:, at(c)], phigh_o.at[:, at(c)], phigh_recv.at[c])

    def own_low(c):
        return pltpu.make_async_copy(low.at[:, at(c)], plow_o.at[:, at(c)], plow_recv.at[c])

    def own_high(c):
        return pltpu.make_async_copy(high.at[:, at(c)], phigh_o.at[:, at(c)], phigh_recv.at[c])

    start_chunks(jnp.logical_not(has_prev), (none_low, none_high), range(CHUNKS))
    start_chunks(all_of(lone, jnp.logical_not(has_low)), (own_low,), BESIDE)
    start_chunks(all_of(lone, jnp.logical_not(has_high)), (own_high,), BESIDE)
    passes = (
        (all_of(lone, qy < 3), pass_up, NEAR),
        (all_of(lone, q == LAYER - 2, above), pass_up, LAST),
        (all_of(lone, qy > 0), pass_down, NEAR),
        (all_of(lone, q == 1, below), pass_down, LAST),
        (all_of(lone, qy == 3, plain_up), pass_up, BESIDE),
        (all_of(lone, qy == 0, plain_down), pass_down, BESIDE),
    )
    only_high, only_low = jnp.logical_and(across, cross_up), jnp.logical_and(across, cross_down)
    not_up = jnp.logical_and(across, jnp.logical_not(cross_up))
    not_down = jnp.logical_and(across, jnp.logical_not(cross_down))
    gifts = (
        ((only_low, give_low, NEAR[:4]), (only_high, give_high, NEAR[:4])),
        (
            (only_low, give_low, NEAR[4:5]),
            (only_high, give_high, NEAR[4:5]),
            (all_of(not_up, not_down, qy == 0), give_low, ACROSS[:1]),
            (all_of(not_up, not_down, qy == 3), give_high, ACROSS[:1]),
            (all_of(not_up, qy > 0), give_low, LAST),
            (all_of(not_down, qy < 3), give_high, LAST),
        ),
        (
            (only_low, give_low, NEAR[5:] + LAST),
            (only_high, give_high, NEAR[5:] + LAST),
            (all_of(not_up, not_down, qy == 0), give_low, ACROSS[1:]),
            (all_of(not_up, not_down, qy == 3), give_high, ACROSS[1:]),
        ),
    )

    def start_gifts(part):
        for there, copy, chunks in gifts[part]:
            start_chunks(there, (copy,), chunks)

    sum_start(*late, 0, partial)
    for there, copy, chunks in passes[:4]:
        start_chunks(there, (copy,), chunks)
    start_gifts(0)
    pl.when(lone)(invert)
    partial = sum_end(*late, 0)
    sum_start(*late, 1, partial)
    for there, copy, chunks in passes[4:]:
        start_chunks(there, (copy,), chunks)
    partial = sum_end(*late, 1)
    sum_start(*late, 2, partial)
    start_gifts(1)
    total[...] = sum_end(*late, 2)
    hand = remote(total.at[pl.ds(n, n // 2)], prior, prior_send, prior_recv, i + 1, r)
    pl.when(has_next)(lambda: hand.start())
    start_gifts(2)
    wait_prior = lambda: pl.when(has_prev)(lambda: hand.wait_recv())
    coefficients(early_total[...], total[...], inv_p[...], prior, wait_prior, w_o, r_o)

    for c in range(CHUNKS):
        give_low(c).wait_recv()
        give_high(c).wait_recv()

    def end_chunks(there, copies, chunks):
        @pl.when(there)
        def _():
            for c in chunks:
                for copy in copies:
                    copy(c).wait_send()

    end_chunks(has_high, (up_plain,), range(CHUNKS))
    end_chunks(has_low, (down_plain,), range(CHUNKS))
    pl.when(has_next)(lambda: hand.wait_send())
    pl.when(has_next)(lambda: early_hand.wait_send())
    end_chunks(has_next, (onward,), range(2 * CHUNKS))
    end_chunks(gives, (give_low, give_high), range(CHUNKS))
    for there, copy, chunks in passes + gifts[0] + gifts[1] + gifts[2]:
        end_chunks(there, (copy,), chunks)
    for there, _, _, copy in first_hops + second_hops:
        pl.when(there)(lambda copy=copy: copy.wait_send())

    for stage in range(3):
        for d in range(1, 4):
            sum_copy(*early, stage, 0, d, r).wait_send()
            sum_copy(*late, stage, 0, d, r).wait_send()


def apply_kernel(
    prev, z_hi, z_lo, plow, phigh, pot, w, r, basis_o, ritz_o, residual_o, out, out_sem, ritz_sem
):
    size = plow.shape[1]
    width = size // CHUNKS
    n = prev.shape[0]
    ritz = pltpu.make_async_copy(r, ritz_o, ritz_sem)
    ritz.start()

    def at(c):
        return pl.ds(pl.multiple_of(c * width, LANES), width)

    def writes(plane, c):
        where = at(plane * CHUNKS + c)
        return [
            pltpu.make_async_copy(out.at[plane, pl.ds(e * n, n)], dst.at[:, where], out_sem.at[plane, e])
            for e, dst in enumerate((basis_o, residual_o))
        ]

    w_hi, w_lo = split(w[...])
    both = jnp.concatenate([w_hi, w_lo], axis=0)

    @pl.loop(0, CHUNKS)
    def _(c):
        for plane in range(2):
            where = at(plane * CHUNKS + c)
            image_hi, image_lo = split(stencil(prev, plow, phigh, pot, plane, c, size, width))
            wide = jnp.dot(
                both, jnp.concatenate([z_hi[:, where], image_hi], axis=0), preferred_element_type=F32
            )
            narrow = jnp.dot(
                w_hi, jnp.concatenate([z_lo[:, where], image_lo], axis=0), preferred_element_type=F32
            )
            value = (wide[: 2 * n] + wide[2 * n :]) + narrow

            @pl.when(c > 0)
            def _():
                for copy in writes(plane, c - 1):
                    copy.wait()

            out[plane] = value
            for copy in writes(plane, c):
                copy.start()

    for plane in range(2):
        for copy in writes(plane, CHUNKS - 1):
            copy.wait()
    ritz.wait()


def solution(mesh):
    intervals, rows = mesh.shape["interval"], mesh.shape["rows"]

    def body(filtered, potential):
        x = filtered[0]
        n, cells = x.shape
        size = cells // 2
        width = size // CHUNKS
        pot = potential.reshape(1, cells)
        hbm = pl.BlockSpec(memory_space=pltpu.HBM)
        vmem = pl.BlockSpec(memory_space=pltpu.VMEM)
        whole = jax.ShapeDtypeStruct((n, cells), F32)
        plane = jax.ShapeDtypeStruct((n, size), F32)
        dma = pltpu.SemaphoreType.DMA

        def kernel(*refs):
            exchange_kernel(intervals, rows, *refs)

        stack = jax.ShapeDtypeStruct((3 * n, cells), BF16)
        prev, z_hi, z_lo, plow, phigh, w, r = pl.pallas_call(
            kernel,
            out_shape=(
                whole, stack, stack, plane, plane,
                jax.ShapeDtypeStruct((2 * n, 4 * n), F32),
                jax.ShapeDtypeStruct((n, n), F32),
            ),
            in_specs=[vmem, vmem],
            out_specs=(vmem,) * 7,
            scratch_shapes=[
                pltpu.VMEM((n, size), F32),
                pltpu.VMEM((n, size), F32),
                *[pltpu.VMEM((n, width), F32) for _ in range(4)],
                pltpu.VMEM((4 * n, 4 * n), F32),
                pltpu.VMEM((3, 4, n + n // 2, 2 * n), F32),
                pltpu.VMEM((n + n // 2, 2 * n), F32),
                pltpu.VMEM((n // 2, 2 * n), F32),
                pltpu.VMEM((3, 4, n // 2, 2 * n), F32),
                pltpu.VMEM((n // 2, 2 * n), F32),
                pltpu.VMEM((n // 2, 2 * n), F32),
                pltpu.VMEM((n, n), F32),
                dma((2 * CHUNKS,)), dma((2 * CHUNKS,)),
                dma((CHUNKS,)), dma((CHUNKS,)), dma((CHUNKS,)), dma((CHUNKS,)),
                dma((4,)), dma((4,)),
                dma((CHUNKS,)), dma((CHUNKS,)),
                dma((CHUNKS,)), dma((CHUNKS,)), dma((CHUNKS,)), dma((CHUNKS,)),
                dma((3, 4)), dma((3, 4)),
                dma, dma,
                dma((3, 4)), dma((3, 4)),
                dma, dma,
            ],
            compiler_params=pltpu.CompilerParams(
                collective_id=0, has_side_effects=True, vmem_limit_bytes=VMEM_EXCHANGE
            ),
            name="exchange",
        )(x, pot)
        basis, ritz, residual = pl.pallas_call(
            apply_kernel,
            out_shape=(whole, jax.ShapeDtypeStruct((n, n), F32), whole),
            in_specs=[vmem] * 8,
            out_specs=(hbm,) * 3,
            scratch_shapes=[pltpu.VMEM((2, 2 * n, width), F32), dma((2, 2)), dma],
            compiler_params=pltpu.CompilerParams(vmem_limit_bytes=VMEM_APPLY),
            name="apply",
        )(prev, z_hi, z_lo, plow, phigh, pot, w, r)
        return basis[None], ritz[None], residual[None]

    return jax.shard_map(
        body,
        mesh=mesh,
        in_specs=(P("interval", None, "rows"), P("rows", None, None)),
        out_specs=(
            P("interval", None, "rows"),
            P("interval", None, None),
            P("interval", None, "rows"),
        ),
        check_vma=False,
    )
```
